32 devices in a mesh: row: 4 (over y, core), col: 8 (over z, x).
Axes of the slice: x: 2, y: 2, z: 4, core: 2. Of those that a mesh axis runs over, the one named last changes fastest.
Arguments:
- factor: float32 [6, 2048, 6, 2048], P(None, 'row', None, 'col'), may hold values from -0.0625 to 0.0625
- diag_inv: float32 [6, 2048, 2048], P(None, None, 'row'), may hold values from -2 to 2, as said below
- structure: int32 [6, 6, 16], P(None, None, 'row'), may hold values 0 or 1
- parent: int32 [6], replicated, may hold values from 1 to 6, as said below
- post: float32 [6, 2048, 64], P(None, 'row', 'col'), may hold values from -6 to 6
Outputs:
- mean_x: float32 [6, 2048, 64], P(None, 'row', 'col')
- variance: float32 [6, 2048], P(None, 'row')
The draws below stay inside these ranges and needn't reach their ends.
Inputs may be any that keep to these rules, and one draw needn't show every extreme that they name: parent[s] > s for s < 5, and parent[5] = 6; every supernode has at most 2 ancestors, and some supernode has exactly that many. The diagonal of each diag_inv[s] lies in 0.5 to 2.
All inputs are finite; a program needn't handle non-finite values. No bound on the sum of `structure` on one device may be relied on, other than what follows from the above.
Results may differ from the reference program's by a relative error of at most 0.00014.
Values sent between devices are 32-bit elements; how exact they have to be, the bound alone decides.
A program may use at most 192 MiB of HBM per device.

```python
import math
import jax
import jax.numpy as jnp
from jax import lax

W = 2048
NSUP = 6
LEVELS = 3
RB = 128
NRHS = 64
NBLK = 16


def draw_diag_inv(key, part):
    key_lower = jax.random.fold_in(key, 11)
    key_diagonal = jax.random.fold_in(key, 12)
    lower_part = jax.random.truncated_normal(key_lower, -4.0, 4.0, (NSUP, W, W), jnp.float32) * (0.5 / math.sqrt(W))
    diagonal = jnp.exp(jax.random.uniform(key_diagonal, (NSUP, W), jnp.float32, math.log(0.5), math.log(2.0)))
    identity = jnp.eye(W, dtype=jnp.float32)
    return lower_part * (1.0 - identity) + diagonal[:, :, None] * identity


def draw_parent(key, part):
    slot_ids = jnp.arange(NSUP + 1, dtype=jnp.int32)
    parent = jnp.full((NSUP,), NSUP, jnp.int32)
    depths = jnp.zeros((NSUP + 1,), jnp.int32)
    for member in range(NSUP - 2, -1, -1):
        if member >= NSUP - LEVELS:
            chosen = jnp.int32(member + 1)
        else:
            eligible = ((slot_ids > member) & (slot_ids < NSUP) & (depths <= LEVELS - 2)).astype(jnp.int32)
            eligible_count = jnp.sum(eligible)
            drawn_slot = jax.random.randint(jax.random.fold_in(key, member), (), 0, eligible_count)
            running = jnp.cumsum(eligible)
            chosen = jnp.argmax((running == drawn_slot + 1) & (eligible == 1)).astype(jnp.int32)
        parent = parent.at[member].set(chosen)
        depths = depths.at[member].set(depths[chosen] + 1)
    return parent


def plant(array, stream_key, low, high):
    spot = [jax.random.randint(jax.random.fold_in(stream_key, axis), (), 0, length) for axis, length in enumerate(array.shape)]
    widest = array.shape.index(max(array.shape))
    neighbour = spot[:widest] + [(spot[widest] + 1) % array.shape[widest]] + spot[widest + 1:]
    return array.at[tuple(spot)].set(low).at[tuple(neighbour)].set(high)


def steps_of(stream_key, dims, shards, smallest, high):
    gain, own = 1.0, jax.random.fold_in(stream_key, 6)
    for position, shards_of in shards:
        draws = jnp.exp(jax.random.uniform(jax.random.fold_in(own, position), (shards_of,), jnp.float32, smallest / len(shards), high / len(shards)))
        gain = gain * jnp.repeat(draws, dims[position] // shards_of).reshape([-1 if axis == position else 1 for axis in range(len(dims))])
    return gain


def gaussian(rng, extent, spread, bound, shards=(), held_as=jnp.bfloat16):
    result = spread * jax.random.normal(rng, extent, jnp.float32)
    if shards:
        result = result * steps_of(rng, extent, shards, -0.22, 0.18)
    return jnp.clip(result, -bound, bound).astype(held_as)


def setup_inputs(seed: int = 0) -> dict:
    key_of = jax.random.split(jax.random.key(seed), 6)
    return {
        "factor": gaussian(key_of[0], (NSUP, W, NSUP, W), (4 * W) ** -0.5, 0.0625, ((1, 4), (3, 8)), jnp.float32),
        "diag_inv": draw_diag_inv(jax.random.fold_in(key_of[5], 71), 0),
        "structure": plant((jax.random.randint(key_of[2], (NSUP, NSUP, NBLK), 0, 4) < 3).astype(jnp.int32), jax.random.fold_in(key_of[2], 1), 0, 1),
        "parent": draw_parent(jax.random.fold_in(key_of[5], 71), 0),
        "post": gaussian(key_of[4], (NSUP, W, NRHS), 1.0, 6.0, ((1, 4), (2, 8)), jnp.float32),
    }


def ancestor_table(parent, super_count):
    extended = jnp.concatenate([parent, jnp.full((1,), super_count, jnp.int32)])
    slot_ids = jnp.arange(super_count + 1, dtype=jnp.int32)
    targets = jnp.arange(super_count, dtype=jnp.int32)
    current = parent
    table = jnp.zeros((super_count, super_count), jnp.float32)
    for hop_index in range(super_count - 1):
        table = table + (current[:, None] == targets[None, :]).astype(jnp.float32)
        onehot = (current[:, None] == slot_ids[None, :]).astype(jnp.int32)
        current = jnp.sum(onehot * extended[None, :], axis=1).astype(jnp.int32)
    return table


def reference(factor, diag_inv, structure, parent, post):
    ancestry = ancestor_table(parent, NSUP)
    row_mask = jnp.repeat(structure.astype(jnp.float32), RB, axis=2) * ancestry[:, :, None]
    lower_inv = jnp.tril(diag_inv)
    order_total = NSUP * W
    solved = [None] * NSUP
    for current_sup in range(NSUP - 1, -1, -1):
        unit_rows = jnp.eye(W, order_total, k=current_sup * W, dtype=jnp.float32)
        right = jnp.concatenate([post[current_sup], unit_rows], axis=1)
        for later in range(current_sup + 1, NSUP):
            block = factor[later, :, current_sup, :] * row_mask[current_sup, later][:, None]
            right = right - jnp.dot(block.T, solved[later], precision=lax.Precision.HIGHEST, preferred_element_type=jnp.float32)
        solved[current_sup] = jnp.dot(lower_inv[current_sup].T, right, precision=lax.Precision.HIGHEST, preferred_element_type=jnp.float32)
    solution = jnp.stack(solved)
    mean_x = solution[:, :, :NRHS]
    unit_part = solution[:, :, NRHS:]
    variance = jnp.sum(unit_part * unit_part, axis=2)
    return mean_x, variance
```

```python
import functools

import jax
import jax.numpy as jnp
from jax import lax
from jax.experimental import pallas as pl
from jax.experimental.pallas import tpu as pltpu
from jax.sharding import PartitionSpec as P

HIGH = lax.Precision.HIGH
MESH = pl.DeviceIdType.MESH
F32 = jnp.float32
BF16 = jnp.bfloat16
VMEM = pltpu.VMEM
VMEM_LIMIT = 64 * 1000 * 1024
CORES = 2
WIDE = 2


def product(left, right):
    return jnp.dot(left, right, precision=HIGH, preferred_element_type=jnp.float32)


def body(factor, diag_inv, structure, parent, post):
    super_count = factor.shape[0]
    row_width = factor.shape[1]
    col_width = factor.shape[3]
    full_width = diag_inv.shape[1]
    row_at = lax.axis_index("row")
    col_at = lax.axis_index("col")
    last = super_count - 1
    block_rows = row_width // structure.shape[2]

    extended = jnp.concatenate([parent, jnp.full((1,), super_count, jnp.int32)])
    first_at = parent
    second_at = extended[parent]

    def pick(current_sup, target):
        clamped = jnp.minimum(target, last)
        block = lax.dynamic_index_in_dim(factor[:, :, current_sup, :], clamped, 0, keepdims=False)
        flags = lax.dynamic_index_in_dim(structure[current_sup], clamped, 0, keepdims=False)
        flags = jnp.where(target < super_count, flags.astype(jnp.float32), 0.0)
        return block * jnp.repeat(flags, block_rows)[:, None]

    blocks = [None] * super_count
    for current_sup in range(last - 1, -1, -1):
        mine = jnp.concatenate(
            [pick(current_sup, first_at[current_sup]), pick(current_sup, second_at[current_sup])], axis=0
        )
        blocks[current_sup] = lax.all_gather(mine, "col", axis=1, tiled=True)

    own_cols = row_at * row_width + jnp.arange(row_width, dtype=jnp.int32)
    rows_full = jnp.arange(full_width, dtype=jnp.int32)
    keep = rows_full[:, None] >= own_cols[None, :]
    lower = [jnp.where(keep, diag_inv[s], 0.0) for s in range(super_count)]
    unit_rows = col_at * col_width + jnp.arange(col_width, dtype=jnp.int32)
    own = lax.dynamic_slice_in_dim(diag_inv, col_at * col_width, col_width, axis=1)
    own = jnp.where((unit_rows[:, None] >= own_cols[None, :])[None], own, 0.0)
    gathered = jnp.swapaxes(lax.all_gather(post, "row", axis=1, tiled=True), 1, 2)

    def take(stacked, target):
        return lax.dynamic_index_in_dim(stacked, jnp.minimum(target, last), 0, keepdims=False)

    rhs = jnp.stack([product(gathered[s], lower[s]) for s in range(super_count)])

    def solve(current_sup, unit_part, rhs_part):
        summed = lax.psum(jnp.concatenate([unit_part, rhs_part], axis=0), "row")
        right = jnp.concatenate(
            [-summed[:col_width], gathered[current_sup] - summed[col_width:]], axis=0
        )
        fresh = product(right, lower[current_sup])
        return fresh[:col_width], fresh[col_width:]

    near = [jnp.zeros((col_width, row_width), jnp.float32)] * super_count
    means = [rhs[s] for s in range(super_count)]
    for s in range(last - 1, -1, -1):
        one, two = first_at[s], second_at[s]
        unit_part = product(take(own, one), blocks[s][:row_width])
        rhs_part = product(
            jnp.concatenate([take(rhs, one), take(rhs, two)], axis=1), blocks[s]
        )
        near[s], means[s] = solve(s, unit_part, rhs_part)
    near_all = jnp.stack(near)
    rhs = jnp.stack(means)

    far = [None] * super_count
    for s in range(last - 1, -1, -1):
        one, two = first_at[s], second_at[s]
        selected = jnp.concatenate(
            [
                jnp.concatenate([take(near_all, one), take(own, two)], axis=1),
                jnp.concatenate([take(rhs, one), take(rhs, two)], axis=1),
            ],
            axis=0,
        )
        both = product(selected, blocks[s])
        far[s], means[s] = solve(s, both[:col_width], both[col_width:])

    squares = []
    for s in range(super_count):
        total = jnp.sum(own[s] * own[s], axis=0)
        if s < last:
            total = total + jnp.sum(near[s] * near[s], axis=0) + jnp.sum(far[s] * far[s], axis=0)
        squares.append(total)
    variance = lax.psum(jnp.stack(squares), "col")
    mean_x = jnp.swapaxes(jnp.stack(means), 1, 2)
    return (mean_x, variance)


def split(x):
    high = x.astype(BF16)
    return high, (x - high.astype(F32)).astype(BF16)


def triple(a, b):
    dot = functools.partial(jnp.dot, preferred_element_type=F32)
    return dot(a[0], b[0]) + (dot(a[0], b[1]) + dot(a[1], b[0]))


def triangle(block, row_start, col_start):
    rows = lax.broadcasted_iota(jnp.int32, block.shape, 0) + row_start
    cols = lax.broadcasted_iota(jnp.int32, block.shape, 1) + col_start
    return jnp.where(rows >= cols, block, 0.0)


def near_partial(targets, diag_inv, blocks):
    count, depth, width = blocks.shape
    full = diag_inv.shape[1]
    parts = full // depth

    def kernel(at, lower, block, out):
        row = lax.axis_index("row")
        right = split(block[0])
        for i in range(parts):
            span = pl.ds(i * depth, depth)

            @pl.when(i >= row)
            def _():
                left = triangle(lower[0, span], i * depth, row * depth)
                out[0, span] = triple(split(left), right)

            @pl.when(i < row)
            def _():
                out[0, span] = jnp.zeros((depth, width), F32)

    return pl.pallas_call(
        kernel,
        grid_spec=pltpu.PrefetchScalarGridSpec(
            num_scalar_prefetch=1,
            grid=(count,),
            in_specs=[
                pl.BlockSpec((1, full, depth), lambda e, at: (at[e], 0, 0)),
                pl.BlockSpec((1, depth, width), lambda e, at: (e, 0, 0)),
            ],
            out_specs=pl.BlockSpec((1, full, width), lambda e, at: (e, 0, 0)),
        ),
        out_shape=jax.ShapeDtypeStruct((count, full, width), F32),
        compiler_params=pltpu.CompilerParams(vmem_limit_bytes=VMEM_LIMIT),
        name="near_partial",
    )(targets, diag_inv, blocks)


def far_partial(slots, targets, valid, near_all, diag_inv, first, second):
    count, depth, width = second.shape
    full = diag_inv.shape[1]
    parts = full // depth
    cols = near_all.shape[0]
    share = depth // cols

    def kernel(slot, at, ok, near, lower, one, two, out):
        e = pl.program_id(0)
        row = lax.axis_index("row")
        left_one = split(jnp.where(ok[e] > 0, one[0], 0.0))
        left_two = split(two[0])
        for i in range(parts):
            span = pl.ds(i * depth, depth)
            rows = near[:, 0, pl.ds(i * share, share)].reshape(depth, depth)
            out[0, span] = triple(split(rows), left_one)

            @pl.when(i >= row)
            def _():
                left = triangle(lower[0, span], i * depth, row * depth)
                out[0, span] += triple(split(left), left_two)

    return pl.pallas_call(
        kernel,
        grid_spec=pltpu.PrefetchScalarGridSpec(
            num_scalar_prefetch=3,
            grid=(count,),
            in_specs=[
                pl.BlockSpec((cols, 1, parts * share, depth), lambda e, slot, at, ok: (0, slot[e], 0, 0)),
                pl.BlockSpec((1, full, depth), lambda e, slot, at, ok: (at[e], 0, 0)),
                pl.BlockSpec((1, depth, width), lambda e, slot, at, ok: (e, 0, 0)),
                pl.BlockSpec((1, depth, width), lambda e, slot, at, ok: (e, 0, 0)),
            ],
            out_specs=pl.BlockSpec((1, full, width), lambda e, slot, at, ok: (e, 0, 0)),
        ),
        out_shape=jax.ShapeDtypeStruct((count, full, width), F32),
        compiler_params=pltpu.CompilerParams(vmem_limit_bytes=VMEM_LIMIT),
        name="far_partial",
    )(slots, targets, valid, near_all, diag_inv, first, second)


def apply_lower(sources, targets, gathered, diag_inv, post, own, steps):
    count, height, full = gathered.shape
    depth = diag_inv.shape[2]
    parts = full // depth
    rhs = post.shape[1]
    share = height // parts
    last = count - 1

    def kernel(at, of, left, lower, post_of, post_own, y, mean, square, total):
        e = pl.program_id(0)
        row = lax.axis_index("row")
        col = lax.axis_index("col")
        mean[0] = jnp.zeros((rhs, depth), F32)
        square[0] = jnp.zeros((8, depth), F32)

        @pl.when(e < count)
        def _():
            total[...] = jnp.zeros_like(total)
            for j in range(parts):
                span = pl.ds(j * depth, depth)

                @pl.when(j >= row)
                def _():
                    right = triangle(lower[0, span], j * depth, row * depth)
                    total[...] += triple(split(left[0, :, span]), split(right))

            found = -total[...]
            y[0] = found
            mean[0] = triple(split(post_of[0]), split(found))
            square[0] = jnp.sum((found * found).reshape(height // 8, 8, depth), axis=0)

        if own:
            for i in range(parts):
                start = i * depth + col * share
                mine = triangle(lower[0, pl.ds(pl.multiple_of(start, 8), share)], start, row * depth)
                total[pl.ds(i * share, share)] = mine
            found_own = total[...]
            mean[0] += triple(split(post_own[0]), split(found_own))
            square[0] += jnp.sum((found_own * found_own).reshape(height // 8, 8, depth), axis=0)

    return pl.pallas_call(
        kernel,
        grid_spec=pltpu.PrefetchScalarGridSpec(
            num_scalar_prefetch=2,
            grid=(steps,),
            in_specs=[
                pl.BlockSpec((1, height, full), lambda e, at, of: (jnp.minimum(e, last), 0, 0)),
                pl.BlockSpec((1, full, depth), lambda e, at, of: (at[e], 0, 0)),
                pl.BlockSpec((1, rhs, height), lambda e, at, of: (of[e], 0, 0)),
                pl.BlockSpec((1, rhs, height), lambda e, at, of: (at[e], 0, 0)),
            ],
            out_specs=[
                pl.BlockSpec((1, height, depth), lambda e, at, of: (jnp.minimum(e, last), 0, 0)),
                pl.BlockSpec((1, rhs, depth), lambda e, at, of: (e, 0, 0)),
                pl.BlockSpec((1, 8, depth), lambda e, at, of: (e, 0, 0)),
            ],
            scratch_shapes=[VMEM((height, depth), F32)],
        ),
        out_shape=[
            jax.ShapeDtypeStruct((count, height, depth), F32),
            jax.ShapeDtypeStruct((steps, rhs, depth), F32),
            jax.ShapeDtypeStruct((steps, 8, depth), F32),
        ],
        compiler_params=pltpu.CompilerParams(vmem_limit_bytes=VMEM_LIMIT),
        name="apply_lower",
    )(sources, targets, gathered, diag_inv, post, post)


def remote(src, dst, send, recv, row, col):
    return pltpu.make_async_remote_copy(
        src_ref=src, dst_ref=dst, send_sem=send, recv_sem=recv, device_id=(row, col), device_id_type=MESH
    )


def redistribute(partial, post, lower_only):
    count, rows, cols, share, width = partial.shape
    tall = rows // CORES
    full = cols * width
    half = full // 2
    with_post = post is not None

    def kernel(*refs):
        d, refs = refs[0], refs[1:]
        if with_post:
            piece, out, posted = refs[:3]
            refs = refs[3:]
        else:
            out = refs[0]
            refs = refs[1:]
        give, own, one, two = refs[:4]
        s1, r1, s2, r2, s3, r3, s4, r4, s5, r5, s6, r6 = refs[4:16]
        row = lax.axis_index("row")
        col = lax.axis_index("col")
        core = row % CORES
        y = row // CORES
        mate = y * CORES + (1 - core)
        across = (1 - y) * CORES + core
        diagonal = (1 - y) * CORES + (1 - core)

        def core_send(e):
            return remote(d.at[e, :, 1 - core], one.at[e], s1.at[e], r1.at[e], mate, col)

        def y_send(e):
            return remote(give.at[e], two.at[e], s2.at[e], r2.at[e], across, col)

        def col_send(e, step):
            to = (col + step) % cols
            return remote(
                own.at[e, to],
                out.at[e, row, :, pl.ds(pl.multiple_of(col * width, 128), width)],
                s3.at[e, step - 1],
                r3.at[e, step - 1],
                row,
                to,
            )

        def mate_send(e):
            return remote(out.at[e, row], out.at[e, row], s4.at[e], r4.at[e], mate, col)

        def upper(e, which):
            return out.at[e, which, :, pl.ds(half, half)]

        def across_full(e):
            return remote(out.at[e, row], out.at[e, row], s5.at[e], r5.at[e], across, col)

        def across_half(e):
            return remote(upper(e, row), upper(e, row), s5.at[e], r5.at[e], across, col)

        def forward_full(e):
            return remote(out.at[e, across], out.at[e, across], s6.at[e], r6.at[e], mate, col)

        def forward_half(e):
            return remote(upper(e, across), upper(e, across), s6.at[e], r6.at[e], mate, col)

        def loop(body):
            def step(e, _):
                body(e)
                return 0

            lax.fori_loop(0, count, step, 0)

        loop(lambda e: core_send(e).start())

        if with_post:
            sp, rp = refs[16:18]

            def post_send(step):
                to_row = (row + step // cols) % rows
                to_col = (col + step % cols) % cols
                return remote(
                    piece.at[to_col], posted.at[row, col], sp.at[step - 1], rp.at[step - 1], to_row, to_col
                )

            posted[row, col] = piece[col]

            def post_start(step, _):
                post_send(step).start()
                return 0

            lax.fori_loop(1, rows * cols, post_start, 0)

        def send_cols(e):
            for step in range(1, cols):
                col_send(e, step).start()
            out[e, row, :, pl.ds(pl.multiple_of(col * width, 128), width)] = own[e, col]

        def first(e):
            core_send(e).wait_recv()
            if lower_only:

                @pl.when(y == 0)
                def _():
                    give[e] = d[e, 1, core] + one[e, 1]
                    y_send(e).start()
                    own[e] = d[e, 0, core] + one[e, 0]
                    send_cols(e)
            else:
                give[e] = d[e, 1 - y, core] + one[e, 1 - y]
                y_send(e).start()

        loop(first)

        def second(e):
            if lower_only:

                @pl.when(y == 1)
                def _():
                    y_send(e).wait_recv()
                    own[e] = d[e, 1, core] + (one[e, 1] + two[e])
                    send_cols(e)
            else:
                y_send(e).wait_recv()
                own[e] = d[e, y, core] + (one[e, y] + two[e])
                send_cols(e)

        loop(second)

        def third(e):
            for step in range(1, cols):
                col_send(e, step).wait_recv()

            @pl.when(y == 0)
            def _():
                across_half(e).start()

            @pl.when(y == 1)
            def _():
                across_full(e).start()

            mate_send(e).start()

        loop(third)

        def fourth(e):
            @pl.when(y == 0)
            def _():
                across_full(e).wait_recv()
                forward_full(e).start()

            @pl.when(y == 1)
            def _():
                across_half(e).wait_recv()
                forward_half(e).start()

        loop(fourth)

        def finish(e):
            core_send(e).wait_send()
            if lower_only:

                @pl.when(y == 0)
                def _():
                    y_send(e).wait_send()
            else:
                y_send(e).wait_send()
            for step in range(1, cols):
                col_send(e, step).wait_send()
            mate_send(e).wait()

            @pl.when(y == 0)
            def _():
                across_half(e).wait_send()
                forward_full(e).wait()

            @pl.when(y == 1)
            def _():
                across_full(e).wait_send()
                forward_half(e).wait()

        loop(finish)

        if with_post:

            def post_wait(step, _):
                post_send(step).wait()
                return 0

            lax.fori_loop(1, rows * cols, post_wait, 0)

    spec = pl.BlockSpec(memory_space=VMEM)
    dma = pltpu.SemaphoreType.DMA
    out_shape = [jax.ShapeDtypeStruct((count, rows, share, full), F32)]
    scratch = [
        VMEM((count, cols, share, width), F32),
        VMEM((count, cols, share, width), F32),
        VMEM((count, tall, cols, share, width), F32),
        VMEM((count, cols, share, width), F32),
    ]
    scratch += [dma((count,))] * 4 + [dma((count, cols - 1))] * 2 + [dma((count,))] * 6
    args = [partial.reshape(count, tall, CORES, cols, share, width)]
    if with_post:
        out_shape.append(jax.ShapeDtypeStruct((rows,) + post.shape, F32))
        scratch += [dma((rows * cols - 1,))] * 2
        args.append(post)
    return pl.pallas_call(
        kernel,
        out_shape=out_shape,
        in_specs=[spec] * len(args),
        out_specs=[spec] * len(out_shape),
        scratch_shapes=scratch,
        compiler_params=pltpu.CompilerParams(vmem_limit_bytes=VMEM_LIMIT, has_side_effects=True),
        name="redistribute",
    )(*args)


def gather_cols(mine, cols):
    count, height, depth = mine.shape
    long = cols // WIDE
    cut = height * 13 // 16 // 8 * 8
    low, high = pl.ds(0, cut), pl.ds(cut, height - cut)

    def kernel(own, out, up_s, up_r, down_s, down_r, x_s, x_r, b_s, b_r):
        row = lax.axis_index("row")
        col = lax.axis_index("col")
        z = col // WIDE
        x = col % WIDE
        peer = z * WIDE + (1 - x)
        spans = [(low, 0), (high, 0), (high, 1)]

        def along(kind, hop, sign):
            span, other = spans[kind]
            block = (z - sign * hop) * WIDE + (x + other) % WIDE
            ref = out.at[block, :, span]
            sems = (up_s, up_r) if sign > 0 else (down_s, down_r)
            return remote(ref, ref, sems[0].at[kind, hop], sems[1].at[kind, hop], row, (z + sign) * WIDE + x)

        def sends(hop, sign):
            return (z - hop >= 0) & (z + 1 < long) if sign > 0 else (z + hop < long) & (z >= 1)

        def gets(hop, sign):
            return z - 1 - hop >= 0 if sign > 0 else z + 1 + hop < long

        def beside(offset):
            block = ((z + offset + long) % long) * WIDE + x
            ref = out.at[block, :, low]
            return remote(ref, ref, x_s.at[offset], x_r.at[offset], row, peer)

        def swap():
            ref = out.at[col, :, high]
            return remote(ref, ref, b_s.at[0], b_r.at[0], row, peer)

        out[col] = own[...]
        swap().start()
        for sign in (1, -1):

            @pl.when(sends(0, sign))
            def _():
                along(0, 0, sign).start()
                along(1, 0, sign).start()

        beside(0).start()
        swap().wait_recv()
        for sign in (1, -1):

            @pl.when(sends(0, sign))
            def _():
                along(2, 0, sign).start()

        for hop in range(long - 1):
            for kind in range(3):
                for sign in (1, -1):

                    @pl.when(gets(hop, sign))
                    def _():
                        along(kind, hop, sign).wait_recv()

                    if hop + 1 < long - 1:

                        @pl.when(sends(hop + 1, sign))
                        def _():
                            along(kind, hop + 1, sign).start()

                    if kind == 0:

                        @pl.when(gets(hop, sign))
                        def _():
                            beside((long - sign * (hop + 1)) % long).start()

        swap().wait_send()
        for offset in range(long):
            beside(offset).wait()
        for hop in range(long - 1):
            for kind in range(3):
                for sign in (1, -1):

                    @pl.when(sends(hop, sign))
                    def _():
                        along(kind, hop, sign).wait_send()

    spec = pl.BlockSpec(memory_space=VMEM)
    dma = pltpu.SemaphoreType.DMA
    return pl.pallas_call(
        kernel,
        out_shape=jax.ShapeDtypeStruct((cols, count, height, depth), F32),
        in_specs=[spec],
        out_specs=spec,
        scratch_shapes=[dma((3, long - 1))] * 4 + [dma((long,))] * 2 + [dma((1,))] * 2,
        compiler_params=pltpu.CompilerParams(vmem_limit_bytes=VMEM_LIMIT, has_side_effects=True),
        name="gather_cols",
    )(mine)


def scatter_sum(parts):
    cols = parts.shape[0]

    def kernel(src, out, landed, send, recv):
        row = lax.axis_index("row")
        col = lax.axis_index("col")

        def copy(step):
            to = (col + step) % cols
            return remote(src.at[to], landed.at[step - 1], send.at[step - 1], recv.at[step - 1], row, to)

        for step in range(1, cols):
            copy(step).start()
        total = src[col]
        for step in range(1, cols):
            copy(step).wait_recv()
            total += landed[step - 1]
        out[...] = total
        for step in range(1, cols):
            copy(step).wait_send()

    spec = pl.BlockSpec(memory_space=VMEM)
    dma = pltpu.SemaphoreType.DMA
    return pl.pallas_call(
        kernel,
        out_shape=jax.ShapeDtypeStruct(parts.shape[1:], F32),
        in_specs=[spec],
        out_specs=spec,
        scratch_shapes=[VMEM((cols - 1,) + parts.shape[1:], F32), dma((cols - 1,)), dma((cols - 1,))],
        compiler_params=pltpu.CompilerParams(vmem_limit_bytes=VMEM_LIMIT, has_side_effects=True),
        name="scatter_sum",
    )(parts)


def fast_body(rows, cols, factor, diag_inv, structure, parent, post):
    supers, row_width, _, col_width = factor.shape
    full = diag_inv.shape[1]
    last = supers - 1
    block_rows = row_width // structure.shape[2]
    share = row_width // cols
    height = rows * share
    rhs_own = post.shape[2]
    rhs = rhs_own * cols
    far_count = supers - 2

    extended = jnp.concatenate([parent, jnp.full((1,), supers, jnp.int32)])
    first_at = parent
    second_at = extended[parent]
    first_clamped = jnp.minimum(first_at, last)
    second_clamped = jnp.minimum(second_at, last)

    def pick(s, target):
        clamped = jnp.minimum(target, last)
        block = lax.dynamic_index_in_dim(factor[:, :, s, :], clamped, 0, keepdims=False)
        flags = lax.dynamic_index_in_dim(structure[s], clamped, 0, keepdims=False)
        flags = jnp.where(target < supers, flags.astype(F32), 0.0)
        return block * jnp.repeat(flags, block_rows)[:, None]

    near_blocks = jnp.stack([pick(s, first_at[s]) for s in range(last)])
    far_blocks = jnp.stack([pick(s, second_at[s]) for s in range(far_count)])

    pieces = jnp.transpose(post.reshape(supers, cols, share, rhs_own), (1, 0, 3, 2))
    pieces = pieces.reshape(cols, supers * rhs_own * share // 128, 128)

    partial = near_partial(first_clamped[:last], diag_inv, near_blocks)
    gathered, posted = redistribute(
        partial.reshape(last, rows, cols, share, col_width), pieces, lower_only=True
    )
    posted = posted.reshape(rows, cols, supers, rhs_own, share)
    posted = jnp.transpose(posted, (2, 1, 3, 0, 4)).reshape(supers, rhs, height)

    order = jnp.arange(supers, dtype=jnp.int32)
    near, means, squares = apply_lower(
        order, first_clamped, gathered.reshape(last, height, full), diag_inv, posted, True, supers
    )

    children = jnp.any(parent[None, :] == order[:, None], axis=1)
    middle = children & (parent < supers)
    mid_low = jnp.argmax(middle).astype(jnp.int32)
    mid_high = (last - jnp.argmax(middle[::-1])).astype(jnp.int32)
    slots = (parent == mid_high).astype(jnp.int32)

    def take(stacked, at):
        return lax.dynamic_index_in_dim(stacked, jnp.minimum(at, last - 1), 0, keepdims=False)

    chosen = jnp.stack([take(near, mid_low), take(near, mid_high)])
    near_all = gather_cols(chosen, cols)

    valid = (second_at < supers).astype(jnp.int32)
    partial = far_partial(
        slots[:far_count], second_clamped[:far_count], valid[:far_count], near_all, diag_inv,
        near_blocks[:far_count], far_blocks,
    )
    (gathered,) = redistribute(partial.reshape(far_count, rows, cols, share, col_width), None, lower_only=False)
    _, far_means, far_squares = apply_lower(
        order[:far_count], second_clamped[:far_count], gathered.reshape(far_count, height, full), diag_inv,
        posted, False, far_count,
    )
    means = means.at[:far_count].add(far_means)
    squares = jnp.sum(squares.at[:far_count].add(far_squares), axis=1)

    by_col = jnp.transpose(means.reshape(supers, cols, rhs_own, row_width), (1, 0, 2, 3))
    by_col = by_col.reshape(cols, supers * rhs_own, row_width)
    pad = -supers % 8
    squares = jnp.concatenate([squares, jnp.zeros((pad, row_width), F32)], axis=0)
    squares = jnp.broadcast_to(squares[None], (cols,) + squares.shape)
    total = scatter_sum(jnp.concatenate([by_col, squares], axis=1))
    mean_rows = supers * rhs_own
    mean_x = jnp.swapaxes(total[:mean_rows].reshape(supers, rhs_own, row_width), 1, 2)
    return mean_x, total[mean_rows : mean_rows + supers]


def solution(mesh):
    rows, cols = mesh.shape["row"], mesh.shape["col"]

    def choose(factor, diag_inv, structure, parent, post):
        shapes_fit = (
            rows == 2 * CORES
            and factor.shape[3] % 128 == 0
            and factor.shape[1] % (8 * cols) == 0
        )
        if shapes_fit:
            return fast_body(rows, cols, factor, diag_inv, structure, parent, post)
        return body(factor, diag_inv, structure, parent, post)

    return jax.shard_map(
        choose,
        mesh=mesh,
        in_specs=(
            P(None, "row", None, "col"),
            P(None, None, "row"),
            P(None, None, "row"),
            P(),
            P(None, "row", "col"),
        ),
        out_specs=(P(None, "row", "col"), P(None, "row")),
        check_vma=False,
    )
```

```python
import functools

import jax
import jax.numpy as jnp
from jax import lax
from jax.experimental import pallas as pl
from jax.experimental.pallas import tpu as pltpu
from jax.sharding import PartitionSpec as P

HIGH = lax.Precision.HIGH
MESH = pl.DeviceIdType.MESH
F32 = jnp.float32
BF16 = jnp.bfloat16
VMEM = pltpu.VMEM
VMEM_LIMIT = 64 * 1000 * 1024
COMPUTE_LIMIT = 64 * 1000 * 1024
CORES = 2
WIDE = 2


def product(left, right):
    return jnp.dot(left, right, precision=HIGH, preferred_element_type=jnp.float32)


def body(factor, diag_inv, structure, parent, post):
    super_count = factor.shape[0]
    row_width = factor.shape[1]
    col_width = factor.shape[3]
    full_width = diag_inv.shape[1]
    row_at = lax.axis_index("row")
    col_at = lax.axis_index("col")
    last = super_count - 1
    block_rows = row_width // structure.shape[2]

    extended = jnp.concatenate([parent, jnp.full((1,), super_count, jnp.int32)])
    first_at = parent
    second_at = extended[parent]

    def pick(current_sup, target):
        clamped = jnp.minimum(target, last)
        block = lax.dynamic_index_in_dim(factor[:, :, current_sup, :], clamped, 0, keepdims=False)
        flags = lax.dynamic_index_in_dim(structure[current_sup], clamped, 0, keepdims=False)
        flags = jnp.where(target < super_count, flags.astype(jnp.float32), 0.0)
        return block * jnp.repeat(flags, block_rows)[:, None]

    blocks = [None] * super_count
    for current_sup in range(last - 1, -1, -1):
        mine = jnp.concatenate(
            [pick(current_sup, first_at[current_sup]), pick(current_sup, second_at[current_sup])], axis=0
        )
        blocks[current_sup] = lax.all_gather(mine, "col", axis=1, tiled=True)

    own_cols = row_at * row_width + jnp.arange(row_width, dtype=jnp.int32)
    rows_full = jnp.arange(full_width, dtype=jnp.int32)
    keep = rows_full[:, None] >= own_cols[None, :]
    lower = [jnp.where(keep, diag_inv[s], 0.0) for s in range(super_count)]
    unit_rows = col_at * col_width + jnp.arange(col_width, dtype=jnp.int32)
    own = lax.dynamic_slice_in_dim(diag_inv, col_at * col_width, col_width, axis=1)
    own = jnp.where((unit_rows[:, None] >= own_cols[None, :])[None], own, 0.0)
    gathered = jnp.swapaxes(lax.all_gather(post, "row", axis=1, tiled=True), 1, 2)

    def take(stacked, target):
        return lax.dynamic_index_in_dim(stacked, jnp.minimum(target, last), 0, keepdims=False)

    rhs = jnp.stack([product(gathered[s], lower[s]) for s in range(super_count)])

    def solve(current_sup, unit_part, rhs_part):
        summed = lax.psum(jnp.concatenate([unit_part, rhs_part], axis=0), "row")
        right = jnp.concatenate(
            [-summed[:col_width], gathered[current_sup] - summed[col_width:]], axis=0
        )
        fresh = product(right, lower[current_sup])
        return fresh[:col_width], fresh[col_width:]

    near = [jnp.zeros((col_width, row_width), jnp.float32)] * super_count
    means = [rhs[s] for s in range(super_count)]
    for s in range(last - 1, -1, -1):
        one, two = first_at[s], second_at[s]
        unit_part = product(take(own, one), blocks[s][:row_width])
        rhs_part = product(
            jnp.concatenate([take(rhs, one), take(rhs, two)], axis=1), blocks[s]
        )
        near[s], means[s] = solve(s, unit_part, rhs_part)
    near_all = jnp.stack(near)
    rhs = jnp.stack(means)

    far = [None] * super_count
    for s in range(last - 1, -1, -1):
        one, two = first_at[s], second_at[s]
        selected = jnp.concatenate(
            [
                jnp.concatenate([take(near_all, one), take(own, two)], axis=1),
                jnp.concatenate([take(rhs, one), take(rhs, two)], axis=1),
            ],
            axis=0,
        )
        both = product(selected, blocks[s])
        far[s], means[s] = solve(s, both[:col_width], both[col_width:])

    squares = []
    for s in range(super_count):
        total = jnp.sum(own[s] * own[s], axis=0)
        if s < last:
            total = total + jnp.sum(near[s] * near[s], axis=0) + jnp.sum(far[s] * far[s], axis=0)
        squares.append(total)
    variance = lax.psum(jnp.stack(squares), "col")
    mean_x = jnp.swapaxes(jnp.stack(means), 1, 2)
    return (mean_x, variance)


def split(x):
    high = x.astype(BF16)
    return high, (x - high.astype(F32)).astype(BF16)


def triple(a, b):
    dot = functools.partial(jnp.dot, preferred_element_type=F32)
    return dot(a[0], b[0]) + (dot(a[0], b[1]) + dot(a[1], b[0]))


def triangle(block, row_start, col_start):
    rows = lax.broadcasted_iota(jnp.int32, block.shape, 0) + row_start
    cols = lax.broadcasted_iota(jnp.int32, block.shape, 1) + col_start
    return jnp.where(rows >= cols, block, 0.0)


FIRST, KEPT, FAR, FAR_TOP, FAR_SLOT, FAR_MID, COUNTS, MIDDLE = 0, 8, 16, 24, 32, 40, 48, 52


def index_tables(parent):
    supers = parent.shape[0]
    last = supers - 1

    def kernel(up, out):
        for i in range(56):
            out[i] = 0
        firsts = [jnp.minimum(up[s], last) for s in range(supers)]
        count = jnp.int32(0)
        low = jnp.int32(last)
        high = jnp.int32(0)
        for s in range(supers):
            out[FIRST + s] = firsts[s]
            out[KEPT + s] = jnp.where(up[s] < supers, 1, 0)
        for s in range(supers):
            far = (up[s] < supers) & (up[firsts[s]] < supers)
            low = jnp.where(far, jnp.minimum(low, firsts[s]), low)
            high = jnp.where(far, jnp.maximum(high, firsts[s]), high)
        for s in range(supers):
            top = up[firsts[s]]
            far = (up[s] < supers) & (top < supers)

            @pl.when(far)
            def _():
                out[FAR + count] = s
                out[FAR_TOP + count] = top
                out[FAR_SLOT + count] = jnp.where(firsts[s] == low, 0, 1)
                out[FAR_MID + count] = firsts[s]

            count = count + jnp.where(far, 1, 0)
        out[COUNTS] = count
        out[COUNTS + 1] = jnp.where(low < high, 2, 1)
        out[MIDDLE] = jnp.minimum(low, last - 1)
        out[MIDDLE + 1] = jnp.minimum(high, last - 1)

    smem = pl.BlockSpec(memory_space=pltpu.SMEM)
    return pl.pallas_call(
        kernel,
        out_shape=jax.ShapeDtypeStruct((56,), jnp.int32),
        in_specs=[smem],
        out_specs=smem,
        name="index_tables",
    )(parent)


def masked(block, flags, s, t, supers, scale):
    depth = block.shape[0]
    pieces = flags.shape[0] // (supers * supers)
    size = depth // pieces
    kept = []
    for b in range(pieces):
        flag = (flags[(s * supers + t) * pieces + b] * scale).astype(F32)
        kept.append(block[b * size : (b + 1) * size] * flag)
    return jnp.concatenate(kept, axis=0)


def near_partial(tables, flags, diag_inv, factor):
    supers, _, depth, width = factor.shape
    full = diag_inv.shape[1]
    parts = full // depth
    count = supers - 1

    def kernel(at, keep, lower, block, out):
        e = pl.program_id(0)
        row = lax.axis_index("row")
        right = split(masked(block[0, 0], keep, e, at[FIRST + e], supers, at[KEPT + e]))
        for i in range(parts):
            span = pl.ds(i * depth, depth)

            @pl.when(i >= row)
            def _():
                left = triangle(lower[0, span], i * depth, row * depth)
                out[0, span] = triple(split(left), right)

            @pl.when(i < row)
            def _():
                out[0, span] = jnp.zeros((depth, width), F32)

    return pl.pallas_call(
        kernel,
        grid_spec=pltpu.PrefetchScalarGridSpec(
            num_scalar_prefetch=2,
            grid=(count,),
            in_specs=[
                pl.BlockSpec((1, full, depth), lambda e, at, keep: (at[FIRST + e], 0, 0)),
                pl.BlockSpec((1, 1, depth, width), lambda e, at, keep: (at[FIRST + e], e, 0, 0)),
            ],
            out_specs=pl.BlockSpec((1, full, width), lambda e, at, keep: (e, 0, 0)),
        ),
        out_shape=jax.ShapeDtypeStruct((count, full, width), F32),
        compiler_params=pltpu.CompilerParams(vmem_limit_bytes=COMPUTE_LIMIT),
        name="near_partial",
    )(tables, flags, diag_inv, factor)


def far_partial(tables, flags, near_all, diag_inv, factor, count):
    supers, _, depth, width = factor.shape
    full = diag_inv.shape[1]
    parts = full // depth
    cols = near_all.shape[0]
    share = depth // cols

    def kernel(at, keep, near, lower, one, two, out):
        e = pl.program_id(0)
        row = lax.axis_index("row")
        s = at[FAR + e]
        left_one = split(masked(one[0, 0], keep, s, at[FAR_MID + e], supers, 1))
        left_two = split(masked(two[0, 0], keep, s, at[FAR_TOP + e], supers, 1))
        for i in range(parts):
            span = pl.ds(i * depth, depth)
            rows = near[:, 0, pl.ds(i * share, share)].reshape(depth, depth)
            out[0, span] = triple(split(rows), left_one)

            @pl.when(i >= row)
            def _():
                left = triangle(lower[0, span], i * depth, row * depth)
                out[0, span] += triple(split(left), left_two)

    return pl.pallas_call(
        kernel,
        grid_spec=pltpu.PrefetchScalarGridSpec(
            num_scalar_prefetch=2,
            grid=(count,),
            in_specs=[
                pl.BlockSpec((cols, 1, parts * share, depth), lambda e, at, keep: (0, at[FAR_SLOT + e], 0, 0)),
                pl.BlockSpec((1, full, depth), lambda e, at, keep: (at[FAR_TOP + e], 0, 0)),
                pl.BlockSpec((1, 1, depth, width), lambda e, at, keep: (at[FAR_MID + e], at[FAR + e], 0, 0)),
                pl.BlockSpec((1, 1, depth, width), lambda e, at, keep: (at[FAR_TOP + e], at[FAR + e], 0, 0)),
            ],
            out_specs=pl.BlockSpec((1, full, width), lambda e, at, keep: (e, 0, 0)),
        ),
        out_shape=jax.ShapeDtypeStruct((count, full, width), F32),
        compiler_params=pltpu.CompilerParams(vmem_limit_bytes=COMPUTE_LIMIT),
        name="far_partial",
    )(tables, flags, near_all, diag_inv, factor, factor)


def square_sum(found):
    return jnp.sum(found * found, axis=0, keepdims=True)


def fill_total(total, left, lower, row):
    depth = lower.shape[2]
    parts = left.shape[2] // depth
    total[...] = jnp.zeros_like(total)
    for j in range(parts):
        span = pl.ds(j * depth, depth)

        @pl.when(j >= row)
        def _():
            right = triangle(lower[0, span], j * depth, row * depth)
            total[...] += triple(split(left[0, :, span]), split(right))


def apply_near(tables, gathered, diag_inv, post):
    count, height, full = gathered.shape
    supers, _, depth = diag_inv.shape
    parts = full // depth
    rhs = post.shape[1]
    share = height // parts
    last = count - 1
    lines = supers + -supers % 8

    def kernel(at, left, lower, post_of, post_own, y, mean, square, total):
        e = pl.program_id(0)
        row = lax.axis_index("row")
        col = lax.axis_index("col")

        for i in range(parts):
            start = i * depth + col * share
            mine = triangle(lower[0, pl.ds(pl.multiple_of(start, 8), share)], start, row * depth)
            total[pl.ds(i * share, share)] = mine
        own = total[...]
        mean[0] = triple(split(post_own[0]), split(own))
        square[pl.ds(e, 1)] = square_sum(own)

        @pl.when(e < count)
        def _():
            fill_total(total, left, lower, row)
            found = -total[...]
            y[0] = found
            mean[0] += triple(split(post_of[0]), split(found))
            square[pl.ds(e, 1)] += square_sum(found)

    return pl.pallas_call(
        kernel,
        grid_spec=pltpu.PrefetchScalarGridSpec(
            num_scalar_prefetch=1,
            grid=(supers,),
            in_specs=[
                pl.BlockSpec((1, height, full), lambda e, at: (jnp.minimum(e, last), 0, 0)),
                pl.BlockSpec((1, full, depth), lambda e, at: (e, 0, 0)),
                pl.BlockSpec((1, rhs, height), lambda e, at: (at[FIRST + e], 0, 0)),
                pl.BlockSpec((1, rhs, height), lambda e, at: (e, 0, 0)),
            ],
            out_specs=[
                pl.BlockSpec((1, height, depth), lambda e, at: (jnp.minimum(e, last), 0, 0)),
                pl.BlockSpec((1, rhs, depth), lambda e, at: (e, 0, 0)),
                pl.BlockSpec((lines, depth), lambda e, at: (0, 0)),
            ],
            scratch_shapes=[VMEM((height, depth), F32)],
        ),
        out_shape=[
            jax.ShapeDtypeStruct((count, height, depth), F32),
            jax.ShapeDtypeStruct((supers, rhs, depth), F32),
            jax.ShapeDtypeStruct((lines, depth), F32),
        ],
        compiler_params=pltpu.CompilerParams(vmem_limit_bytes=COMPUTE_LIMIT),
        name="apply_near",
    )(tables, gathered, diag_inv, post, post)


def apply_far(tables, gathered, diag_inv, post, mean, square):
    count, height, full = gathered.shape
    _, _, depth = diag_inv.shape
    rhs = post.shape[1]

    def kernel(at, left, lower, post_of, mean_in, square_in, mean_out, square_out, total):
        e = pl.program_id(0)
        row = lax.axis_index("row")

        @pl.when(e == 0)
        def _():
            square_out[...] = square_in[...]

        fill_total(total, left, lower, row)
        found = -total[...]
        mean_out[0] = mean_in[0] + triple(split(post_of[0]), split(found))
        square_out[pl.ds(at[FAR + e], 1)] += square_sum(found)

    mean_spec = pl.BlockSpec((1, rhs, depth), lambda e, at: (at[FAR + e], 0, 0))
    square_spec = pl.BlockSpec(square.shape, lambda e, at: (0, 0))
    return pl.pallas_call(
        kernel,
        grid_spec=pltpu.PrefetchScalarGridSpec(
            num_scalar_prefetch=1,
            grid=(count,),
            in_specs=[
                pl.BlockSpec((1, height, full), lambda e, at: (e, 0, 0)),
                pl.BlockSpec((1, full, depth), lambda e, at: (at[FAR + e], 0, 0)),
                pl.BlockSpec((1, rhs, height), lambda e, at: (at[FAR_TOP + e], 0, 0)),
                mean_spec,
                square_spec,
            ],
            out_specs=[mean_spec, square_spec],
            scratch_shapes=[VMEM((height, depth), F32)],
        ),
        out_shape=[
            jax.ShapeDtypeStruct(mean.shape, F32),
            jax.ShapeDtypeStruct(square.shape, F32),
        ],
        input_output_aliases={4: 0, 5: 1},
        compiler_params=pltpu.CompilerParams(vmem_limit_bytes=COMPUTE_LIMIT),
        name="apply_far",
    )(tables, gathered, diag_inv, post, mean, square)


def remote(src, dst, send, recv, row, col):
    return pltpu.make_async_remote_copy(
        src_ref=src, dst_ref=dst, send_sem=send, recv_sem=recv, device_id=(row, col), device_id_type=MESH
    )


def redistribute(partial, post, lower_only):
    count, rows, cols, share, width = partial.shape
    tall = rows // CORES
    full = cols * width
    half = full // 2
    with_post = post is not None

    def kernel(*refs):
        d, refs = refs[0], refs[1:]
        if with_post:
            piece, out, posted = refs[:3]
            refs = refs[3:]
        else:
            out = refs[0]
            refs = refs[1:]
        give, own, one, two = refs[:4]
        s1, r1, s2, r2, s3, r3, s4, r4, s5, r5, s6, r6 = refs[4:16]
        row = lax.axis_index("row")
        col = lax.axis_index("col")
        core = row % CORES
        y = row // CORES
        mate = y * CORES + (1 - core)
        across = (1 - y) * CORES + core
        diagonal = (1 - y) * CORES + (1 - core)

        def core_send(e):
            return remote(d.at[e, :, 1 - core], one.at[e], s1.at[e], r1.at[e], mate, col)

        def y_send(e):
            return remote(give.at[e], two.at[e], s2.at[e], r2.at[e], across, col)

        def col_send(e, step):
            to = (col + step) % cols
            return remote(
                own.at[e, to],
                out.at[e, row, :, pl.ds(pl.multiple_of(col * width, 128), width)],
                s3.at[e, step - 1],
                r3.at[e, step - 1],
                row,
                to,
            )

        def mate_send(e):
            return remote(out.at[e, row], out.at[e, row], s4.at[e], r4.at[e], mate, col)

        def upper(e, which):
            return out.at[e, which, :, pl.ds(half, half)]

        def across_full(e):
            return remote(out.at[e, row], out.at[e, row], s5.at[e], r5.at[e], across, col)

        def across_half(e):
            return remote(upper(e, row), upper(e, row), s5.at[e], r5.at[e], across, col)

        def forward_full(e):
            return remote(out.at[e, across], out.at[e, across], s6.at[e], r6.at[e], mate, col)

        def forward_half(e):
            return remote(upper(e, across), upper(e, across), s6.at[e], r6.at[e], mate, col)

        def loop(body):
            def step(e, _):
                body(e)
                return 0

            lax.fori_loop(0, count, step, 0)

        loop(lambda e: core_send(e).start())

        if with_post:
            sp, rp = refs[16:18]

            def post_send(step):
                to_row = (row + step // cols) % rows
                to_col = (col + step % cols) % cols
                return remote(
                    piece.at[to_col], posted.at[row, col], sp.at[step - 1], rp.at[step - 1], to_row, to_col
                )

            posted[row, col] = piece[col]

            def post_start(step, _):
                post_send(step).start()
                return 0

            lax.fori_loop(1, rows * cols, post_start, 0)

        def send_cols(e):
            for step in range(1, cols):
                col_send(e, step).start()
            out[e, row, :, pl.ds(pl.multiple_of(col * width, 128), width)] = own[e, col]

        def first(e):
            core_send(e).wait_recv()
            if lower_only:

                @pl.when(y == 0)
                def _():
                    give[e] = d[e, 1, core] + one[e, 1]
                    y_send(e).start()
                    own[e] = d[e, 0, core] + one[e, 0]
                    send_cols(e)
            else:
                give[e] = d[e, 1 - y, core] + one[e, 1 - y]
                y_send(e).start()

        def second(e):
            if lower_only:

                @pl.when(y == 1)
                def _():
                    y_send(e).wait_recv()
                    own[e] = d[e, 1, core] + (one[e, 1] + two[e])
                    send_cols(e)
            else:
                y_send(e).wait_recv()
                own[e] = d[e, y, core] + (one[e, y] + two[e])
                send_cols(e)

        def third(e):
            for step in range(1, cols):
                col_send(e, step).wait_recv()

            @pl.when(y == 0)
            def _():
                across_half(e).start()

            @pl.when(y == 1)
            def _():
                across_full(e).start()

            mate_send(e).start()

        def fourth(e):
            @pl.when(y == 0)
            def _():
                across_full(e).wait_recv()
                forward_full(e).start()

            @pl.when(y == 1)
            def _():
                across_half(e).wait_recv()
                forward_half(e).start()

        loop(first)

        def stages(t, _):
            for lag, stage in enumerate((second, third, fourth)):

                @pl.when((t >= lag) & (t < count + lag))
                def _():
                    stage(t - lag)

            return 0

        lax.fori_loop(0, count + 2, stages, 0)

        def finish(e):
            core_send(e).wait_send()
            if lower_only:

                @pl.when(y == 0)
                def _():
                    y_send(e).wait_send()
            else:
                y_send(e).wait_send()
            for step in range(1, cols):
                col_send(e, step).wait_send()
            mate_send(e).wait()

            @pl.when(y == 0)
            def _():
                across_half(e).wait_send()
                forward_full(e).wait()

            @pl.when(y == 1)
            def _():
                across_full(e).wait_send()
                forward_half(e).wait()

        loop(finish)

        if with_post:

            def post_wait(step, _):
                post_send(step).wait()
                return 0

            lax.fori_loop(1, rows * cols, post_wait, 0)

    spec = pl.BlockSpec(memory_space=VMEM)
    dma = pltpu.SemaphoreType.DMA
    out_shape = [jax.ShapeDtypeStruct((count, rows, share, full), F32)]
    scratch = [
        VMEM((count, cols, share, width), F32),
        VMEM((count, cols, share, width), F32),
        VMEM((count, tall, cols, share, width), F32),
        VMEM((count, cols, share, width), F32),
    ]
    scratch += [dma((count,))] * 4 + [dma((count, cols - 1))] * 2 + [dma((count,))] * 6
    args = [partial.reshape(count, tall, CORES, cols, share, width)]
    if with_post:
        out_shape.append(jax.ShapeDtypeStruct((rows,) + post.shape, F32))
        scratch += [dma((rows * cols - 1,))] * 2
        args.append(post)
    return pl.pallas_call(
        kernel,
        out_shape=out_shape,
        in_specs=[spec] * len(args),
        out_specs=[spec] * len(out_shape),
        scratch_shapes=scratch,
        compiler_params=pltpu.CompilerParams(vmem_limit_bytes=VMEM_LIMIT, has_side_effects=True),
        name="redistribute",
    )(*args)


def gather_cols(tables, near, cols, count):
    _, height, depth = near.shape
    long = cols // WIDE
    cut = height * 13 // 16 // 8 * 8
    low, high = pl.ds(0, cut), pl.ds(cut, height - cut)
    spans = [(low, 0), (high, 0), (high, 1)]

    def kernel(at, near_ref, out, up_s, up_r, down_s, down_r, x_s, x_r, b_s, b_r):
        row = lax.axis_index("row")
        col = lax.axis_index("col")
        z = col // WIDE
        x = col % WIDE
        peer = z * WIDE + (1 - x)

        def along(p, kind, hop, sign):
            span, other = spans[kind]
            block = (z - sign * hop) * WIDE + (x + other) % WIDE
            ref = out.at[block, p, span]
            sems = (up_s, up_r) if sign > 0 else (down_s, down_r)
            return remote(ref, ref, sems[0].at[p, kind, hop], sems[1].at[p, kind, hop], row, (z + sign) * WIDE + x)

        def sends(hop, sign):
            return (z - hop >= 0) & (z + 1 < long) if sign > 0 else (z + hop < long) & (z >= 1)

        def gets(hop, sign):
            return z - 1 - hop >= 0 if sign > 0 else z + 1 + hop < long

        def beside(p, offset):
            block = ((z + offset + long) % long) * WIDE + x
            ref = out.at[block, p, low]
            return remote(ref, ref, x_s.at[p, offset], x_r.at[p, offset], row, peer)

        def swap(p):
            ref = out.at[col, p, high]
            return remote(ref, ref, b_s.at[p], b_r.at[p], row, peer)

        for p in range(count):
            out[col, p] = near_ref[at[MIDDLE + p]]
            swap(p).start()
            for sign in (1, -1):

                @pl.when(sends(0, sign))
                def _():
                    along(p, 0, 0, sign).start()
                    along(p, 1, 0, sign).start()

            beside(p, 0).start()
        for p in range(count):
            swap(p).wait_recv()
            for sign in (1, -1):

                @pl.when(sends(0, sign))
                def _():
                    along(p, 2, 0, sign).start()

        for hop in range(long - 1):
            for p in range(count):
                for kind in range(3):
                    for sign in (1, -1):

                        @pl.when(gets(hop, sign))
                        def _():
                            along(p, kind, hop, sign).wait_recv()

                        if hop + 1 < long - 1:

                            @pl.when(sends(hop + 1, sign))
                            def _():
                                along(p, kind, hop + 1, sign).start()

                        if kind == 0:

                            @pl.when(gets(hop, sign))
                            def _():
                                beside(p, (long - sign * (hop + 1)) % long).start()

        for p in range(count):
            swap(p).wait_send()
            for offset in range(long):
                beside(p, offset).wait()
            for hop in range(long - 1):
                for kind in range(3):
                    for sign in (1, -1):

                        @pl.when(sends(hop, sign))
                        def _():
                            along(p, kind, hop, sign).wait_send()

    spec = pl.BlockSpec(memory_space=VMEM)
    dma = pltpu.SemaphoreType.DMA
    return pl.pallas_call(
        kernel,
        out_shape=jax.ShapeDtypeStruct((cols, 2, height, depth), F32),
        in_specs=[pl.BlockSpec(memory_space=pltpu.SMEM), spec],
        out_specs=spec,
        scratch_shapes=[dma((count, 3, long - 1))] * 4 + [dma((count, long))] * 2 + [dma((count,))] * 2,
        compiler_params=pltpu.CompilerParams(vmem_limit_bytes=VMEM_LIMIT, has_side_effects=True),
        name="gather_cols",
    )(tables, near)


def scatter_sum(mean, square, cols):
    supers, rhs, depth = mean.shape
    own = rhs // cols

    def kernel(src, sq, out, sq_out, landed, sq_landed, send, recv, sq_send, sq_recv):
        row = lax.axis_index("row")
        col = lax.axis_index("col")

        def piece(c):
            return pl.ds(pl.multiple_of(c * own, own), own)

        def copy(step):
            to = (col + step) % cols
            return remote(
                src.at[:, piece(to)], landed.at[step - 1], send.at[step - 1], recv.at[step - 1], row, to
            )

        def sq_copy(step):
            to = (col + step) % cols
            return remote(sq, sq_landed.at[step - 1], sq_send.at[step - 1], sq_recv.at[step - 1], row, to)

        for step in range(1, cols):
            copy(step).start()
            sq_copy(step).start()
        total = src[:, piece(col)]
        sq_total = sq[...]
        for step in range(1, cols):
            copy(step).wait_recv()
            sq_copy(step).wait_recv()
            total += landed[step - 1]
            sq_total += sq_landed[step - 1]
        out[...] = total
        sq_out[...] = sq_total
        for step in range(1, cols):
            copy(step).wait_send()
            sq_copy(step).wait_send()

    spec = pl.BlockSpec(memory_space=VMEM)
    dma = pltpu.SemaphoreType.DMA
    return pl.pallas_call(
        kernel,
        out_shape=[
            jax.ShapeDtypeStruct((supers, own, depth), F32),
            jax.ShapeDtypeStruct(square.shape, F32),
        ],
        in_specs=[spec, spec],
        out_specs=[spec, spec],
        scratch_shapes=[
            VMEM((cols - 1, supers, own, depth), F32),
            VMEM((cols - 1,) + square.shape, F32),
        ]
        + [dma((cols - 1,))] * 4,
        compiler_params=pltpu.CompilerParams(vmem_limit_bytes=VMEM_LIMIT, has_side_effects=True),
        name="scatter_sum",
    )(mean, square)


def fast_body(rows, cols, factor, diag_inv, structure, parent, post):
    supers, row_width, _, col_width = factor.shape
    full = diag_inv.shape[1]
    last = supers - 1
    share = row_width // cols
    height = rows * share
    rhs_own = post.shape[2]
    rhs = rhs_own * cols

    tables = index_tables(parent)
    flags = structure.reshape(-1)
    blocks = jnp.transpose(factor, (0, 2, 1, 3))

    pieces = jnp.transpose(post.reshape(supers, cols, share, rhs_own), (1, 0, 3, 2))
    pieces = pieces.reshape(cols, supers * rhs_own * share // 128, 128)

    partial = near_partial(tables, flags, diag_inv, blocks)
    gathered, posted = redistribute(
        partial.reshape(last, rows, cols, share, col_width), pieces, lower_only=True
    )
    posted = posted.reshape(rows, cols, supers, rhs_own, share)
    posted = jnp.transpose(posted, (2, 1, 3, 0, 4)).reshape(supers, rhs, height)
    near, mean, square = apply_near(tables, gathered.reshape(last, height, full), diag_inv, posted)

    gathers = [functools.partial(gather_cols, cols=cols, count=count) for count in (1, 2)]
    near_all = lax.switch(tables[COUNTS + 1] - 1, gathers, tables, near)

    def far_steps(count, tables, near_all, mean, square):
        partial = far_partial(tables, flags, near_all, diag_inv, blocks, count)
        (gathered,) = redistribute(
            partial.reshape(count, rows, cols, share, col_width), None, lower_only=False
        )
        return apply_far(tables, gathered.reshape(count, height, full), diag_inv, posted, mean, square)

    counts = [functools.partial(far_steps, count) for count in range(1, supers - 1)]
    mean, square = lax.switch(tables[COUNTS] - 1, counts, tables, near_all, mean, square)
    mean, square = scatter_sum(mean, square, cols)
    return jnp.swapaxes(mean, 1, 2), square[:supers]


def solution(mesh):
    rows, cols = mesh.shape["row"], mesh.shape["col"]

    def choose(factor, diag_inv, structure, parent, post):
        shapes_fit = (
            rows == 2 * CORES
            and factor.shape[3] % 128 == 0
            and factor.shape[1] % (8 * cols) == 0
            and post.shape[2] % 8 == 0
        )
        if shapes_fit:
            return fast_body(rows, cols, factor, diag_inv, structure, parent, post)
        return body(factor, diag_inv, structure, parent, post)

    return jax.shard_map(
        choose,
        mesh=mesh,
        in_specs=(
            P(None, "row", None, "col"),
            P(None, None, "row"),
            P(None, None, "row"),
            P(),
            P(None, "row", "col"),
        ),
        out_specs=(P(None, "row", "col"), P(None, "row")),
        check_vma=False,
    )
```

```python
import functools

import jax
import jax.numpy as jnp
from jax import lax
from jax.experimental import pallas as pl
from jax.experimental.pallas import tpu as pltpu
from jax.sharding import PartitionSpec as P

HIGH = lax.Precision.HIGH
MESH = pl.DeviceIdType.MESH
F32 = jnp.float32
BF16 = jnp.bfloat16
VMEM = pltpu.VMEM
VMEM_LIMIT = 64 * 1000 * 1024
COMPUTE_LIMIT = 64 * 1000 * 1024
CORES = 2
WIDE = 2


def product(left, right):
    return jnp.dot(left, right, precision=HIGH, preferred_element_type=jnp.float32)


def body(factor, diag_inv, structure, parent, post):
    super_count = factor.shape[0]
    row_width = factor.shape[1]
    col_width = factor.shape[3]
    full_width = diag_inv.shape[1]
    row_at = lax.axis_index("row")
    col_at = lax.axis_index("col")
    last = super_count - 1
    block_rows = row_width // structure.shape[2]

    extended = jnp.concatenate([parent, jnp.full((1,), super_count, jnp.int32)])
    first_at = parent
    second_at = extended[parent]

    def pick(current_sup, target):
        clamped = jnp.minimum(target, last)
        block = lax.dynamic_index_in_dim(factor[:, :, current_sup, :], clamped, 0, keepdims=False)
        flags = lax.dynamic_index_in_dim(structure[current_sup], clamped, 0, keepdims=False)
        flags = jnp.where(target < super_count, flags.astype(jnp.float32), 0.0)
        return block * jnp.repeat(flags, block_rows)[:, None]

    blocks = [None] * super_count
    for current_sup in range(last - 1, -1, -1):
        mine = jnp.concatenate(
            [pick(current_sup, first_at[current_sup]), pick(current_sup, second_at[current_sup])], axis=0
        )
        blocks[current_sup] = lax.all_gather(mine, "col", axis=1, tiled=True)

    own_cols = row_at * row_width + jnp.arange(row_width, dtype=jnp.int32)
    rows_full = jnp.arange(full_width, dtype=jnp.int32)
    keep = rows_full[:, None] >= own_cols[None, :]
    lower = [jnp.where(keep, diag_inv[s], 0.0) for s in range(super_count)]
    unit_rows = col_at * col_width + jnp.arange(col_width, dtype=jnp.int32)
    own = lax.dynamic_slice_in_dim(diag_inv, col_at * col_width, col_width, axis=1)
    own = jnp.where((unit_rows[:, None] >= own_cols[None, :])[None], own, 0.0)
    gathered = jnp.swapaxes(lax.all_gather(post, "row", axis=1, tiled=True), 1, 2)

    def take(stacked, target):
        return lax.dynamic_index_in_dim(stacked, jnp.minimum(target, last), 0, keepdims=False)

    rhs = jnp.stack([product(gathered[s], lower[s]) for s in range(super_count)])

    def solve(current_sup, unit_part, rhs_part):
        summed = lax.psum(jnp.concatenate([unit_part, rhs_part], axis=0), "row")
        right = jnp.concatenate(
            [-summed[:col_width], gathered[current_sup] - summed[col_width:]], axis=0
        )
        fresh = product(right, lower[current_sup])
        return fresh[:col_width], fresh[col_width:]

    near = [jnp.zeros((col_width, row_width), jnp.float32)] * super_count
    means = [rhs[s] for s in range(super_count)]
    for s in range(last - 1, -1, -1):
        one, two = first_at[s], second_at[s]
        unit_part = product(take(own, one), blocks[s][:row_width])
        rhs_part = product(
            jnp.concatenate([take(rhs, one), take(rhs, two)], axis=1), blocks[s]
        )
        near[s], means[s] = solve(s, unit_part, rhs_part)
    near_all = jnp.stack(near)
    rhs = jnp.stack(means)

    far = [None] * super_count
    for s in range(last - 1, -1, -1):
        one, two = first_at[s], second_at[s]
        selected = jnp.concatenate(
            [
                jnp.concatenate([take(near_all, one), take(own, two)], axis=1),
                jnp.concatenate([take(rhs, one), take(rhs, two)], axis=1),
            ],
            axis=0,
        )
        both = product(selected, blocks[s])
        far[s], means[s] = solve(s, both[:col_width], both[col_width:])

    squares = []
    for s in range(super_count):
        total = jnp.sum(own[s] * own[s], axis=0)
        if s < last:
            total = total + jnp.sum(near[s] * near[s], axis=0) + jnp.sum(far[s] * far[s], axis=0)
        squares.append(total)
    variance = lax.psum(jnp.stack(squares), "col")
    mean_x = jnp.swapaxes(jnp.stack(means), 1, 2)
    return (mean_x, variance)


def split(x):
    high = x.astype(BF16)
    return high, (x - high.astype(F32)).astype(BF16)


def triple(a, b):
    dot = functools.partial(jnp.dot, preferred_element_type=F32)
    return dot(a[0], b[0]) + (dot(a[0], b[1]) + dot(a[1], b[0]))


def triangle(block, row_start, col_start):
    rows = lax.broadcasted_iota(jnp.int32, block.shape, 0) + row_start
    cols = lax.broadcasted_iota(jnp.int32, block.shape, 1) + col_start
    return jnp.where(rows >= cols, block, 0.0)


FIRST, KEPT, FAR, FAR_TOP, FAR_SLOT, FAR_MID, NEAR, NEAR_TOP, COUNTS = 0, 8, 16, 24, 32, 40, 48, 56, 64


def index_tables(parent):
    supers = parent.shape[0]
    last = supers - 1

    def kernel(up, out):
        for i in range(72):
            out[i] = 0
        firsts = [jnp.minimum(up[s], last) for s in range(supers)]
        count = jnp.int32(0)
        low = jnp.int32(last)
        high = jnp.int32(0)
        for s in range(supers):
            out[FIRST + s] = firsts[s]
            out[KEPT + s] = jnp.where(up[s] < supers, 1, 0)
        for s in range(supers):
            far = (up[s] < supers) & (up[firsts[s]] < supers)
            low = jnp.where(far, jnp.minimum(low, firsts[s]), low)
            high = jnp.where(far, jnp.maximum(high, firsts[s]), high)
        for s in range(supers):
            top = up[firsts[s]]
            far = (up[s] < supers) & (top < supers)

            @pl.when(far)
            def _():
                out[FAR + count] = s
                out[FAR_TOP + count] = top
                out[FAR_SLOT + count] = jnp.where(firsts[s] == low, 0, 1)
                out[FAR_MID + count] = firsts[s]

            count = count + jnp.where(far, 1, 0)
        out[COUNTS] = count
        out[COUNTS + 1] = jnp.where(low < high, 2, 1)
        out[COUNTS + 2] = lax.axis_index("col")
        place = jnp.int32(0)
        for middle in (True, False):
            for s in range(last):
                between = (low == s) | (high == s)
                now = between if middle else jnp.logical_not(between)

                @pl.when(now)
                def _():
                    out[NEAR + place] = s
                    out[NEAR_TOP + place] = firsts[s]

                place = place + jnp.where(now, 1, 0)

    smem = pl.BlockSpec(memory_space=pltpu.SMEM)
    return pl.pallas_call(
        kernel,
        out_shape=jax.ShapeDtypeStruct((72,), jnp.int32),
        in_specs=[smem],
        out_specs=smem,
        name="index_tables",
    )(parent)


def masked(block, flags, s, t, supers, scale):
    depth = block.shape[0]
    pieces = flags.shape[0] // (supers * supers)
    size = depth // pieces
    kept = []
    for b in range(pieces):
        flag = (flags[(s * supers + t) * pieces + b] * scale).astype(F32)
        kept.append(block[b * size : (b + 1) * size] * flag)
    return jnp.concatenate(kept, axis=0)


def near_partial(tables, flags, diag_inv, factor):
    supers, _, depth, width = factor.shape
    full = diag_inv.shape[1]
    parts = full // depth
    count = supers - 1

    def kernel(at, keep, lower, block, out):
        e = pl.program_id(0)
        row = lax.axis_index("row")
        s = at[NEAR + e]
        right = split(masked(block[0, 0], keep, s, at[NEAR_TOP + e], supers, at[KEPT + s]))

        def below(i, _):
            span = pl.ds(pl.multiple_of(i * depth, 8), depth)
            left = triangle(lower[0, span], i * depth, row * depth)
            out[0, span] = triple(split(left), right)
            return 0

        def above(i, _):
            span = pl.ds(pl.multiple_of(i * depth, 8), depth)
            out[0, span] = jnp.zeros((depth, width), F32)
            return 0

        lax.fori_loop(row, parts, below, 0)
        lax.fori_loop(0, row, above, 0)

    return pl.pallas_call(
        kernel,
        grid_spec=pltpu.PrefetchScalarGridSpec(
            num_scalar_prefetch=2,
            grid=(count,),
            in_specs=[
                pl.BlockSpec((1, full, depth), lambda e, at, keep: (at[NEAR_TOP + e], 0, 0)),
                pl.BlockSpec((1, 1, depth, width), lambda e, at, keep: (at[NEAR_TOP + e], at[NEAR + e], 0, 0)),
            ],
            out_specs=pl.BlockSpec((1, full, width), lambda e, at, keep: (e, 0, 0)),
        ),
        out_shape=jax.ShapeDtypeStruct((count, full, width), F32),
        compiler_params=pltpu.CompilerParams(vmem_limit_bytes=COMPUTE_LIMIT),
        name="near_partial",
    )(tables, flags, diag_inv, factor)


def far_partial(tables, flags, near_all, diag_inv, factor, count):
    supers, _, depth, width = factor.shape
    full = diag_inv.shape[1]
    parts = full // depth
    cols = near_all.shape[0]
    share = depth // cols

    def kernel(at, keep, near, lower, one, two, out):
        e = pl.program_id(0)
        row = lax.axis_index("row")
        s = at[FAR + e]
        left_one = split(masked(one[0, 0], keep, s, at[FAR_MID + e], supers, 1))
        left_two = split(masked(two[0, 0], keep, s, at[FAR_TOP + e], supers, 1))

        def dense(i, _):
            span = pl.ds(pl.multiple_of(i * depth, 8), depth)
            rows = near[:, 0, pl.ds(pl.multiple_of(i * share, 8), share)].reshape(depth, depth)
            out[0, span] = triple(split(rows), left_one)
            return 0

        def below(i, _):
            span = pl.ds(pl.multiple_of(i * depth, 8), depth)
            left = triangle(lower[0, span], i * depth, row * depth)
            out[0, span] += triple(split(left), left_two)
            return 0

        lax.fori_loop(0, parts, dense, 0)
        lax.fori_loop(row, parts, below, 0)

    return pl.pallas_call(
        kernel,
        grid_spec=pltpu.PrefetchScalarGridSpec(
            num_scalar_prefetch=2,
            grid=(count,),
            in_specs=[
                pl.BlockSpec((cols, 1, parts * share, depth), lambda e, at, keep: (0, at[FAR_SLOT + e], 0, 0)),
                pl.BlockSpec((1, full, depth), lambda e, at, keep: (at[FAR_TOP + e], 0, 0)),
                pl.BlockSpec((1, 1, depth, width), lambda e, at, keep: (at[FAR_MID + e], at[FAR + e], 0, 0)),
                pl.BlockSpec((1, 1, depth, width), lambda e, at, keep: (at[FAR_TOP + e], at[FAR + e], 0, 0)),
            ],
            out_specs=pl.BlockSpec((1, full, width), lambda e, at, keep: (e, 0, 0)),
        ),
        out_shape=jax.ShapeDtypeStruct((count, full, width), F32),
        compiler_params=pltpu.CompilerParams(vmem_limit_bytes=COMPUTE_LIMIT),
        name="far_partial",
    )(tables, flags, near_all, diag_inv, factor, factor)


def square_sum(found):
    return jnp.sum(found * found, axis=0, keepdims=True)


def fill_total(total, left, lower, row):
    depth = lower.shape[2]
    parts = left.shape[2] // depth
    total[...] = jnp.zeros_like(total)

    def add(j, _):
        span = pl.ds(pl.multiple_of(j * depth, 128), depth)
        right = triangle(lower[0, span], j * depth, row * depth)
        total[...] += triple(split(left[0, :, span]), split(right))
        return 0

    lax.fori_loop(row, parts, add, 0)


def own_terms(tables, diag_inv, post):
    supers, full, depth = diag_inv.shape
    _, rhs, height = post.shape
    parts = full // depth
    share = height // parts
    cols = depth // share
    lines = supers + -supers % 8

    def kernel(at, lower, post_own, mean, square):
        e = pl.program_id(0)
        row = lax.axis_index("row")
        col = lax.axis_index("col")
        rows = [
            triangle(lower[0, i, 0], i * depth + col * share, row * depth) for i in range(parts)
        ]
        own = jnp.concatenate(rows, axis=0)
        mean[0] = triple(split(post_own[0]), split(own))
        square[pl.ds(e, 1)] = square_sum(own)

    return pl.pallas_call(
        kernel,
        grid_spec=pltpu.PrefetchScalarGridSpec(
            num_scalar_prefetch=1,
            grid=(supers,),
            in_specs=[
                pl.BlockSpec((1, parts, 1, share, depth), lambda e, at: (e, 0, at[COUNTS + 2], 0, 0)),
                pl.BlockSpec((1, rhs, height), lambda e, at: (e, 0, 0)),
            ],
            out_specs=[
                pl.BlockSpec((1, rhs, depth), lambda e, at: (e, 0, 0)),
                pl.BlockSpec((lines, depth), lambda e, at: (0, 0)),
            ],
        ),
        out_shape=[
            jax.ShapeDtypeStruct((supers, rhs, depth), F32),
            jax.ShapeDtypeStruct((lines, depth), F32),
        ],
        compiler_params=pltpu.CompilerParams(vmem_limit_bytes=COMPUTE_LIMIT),
        name="own_terms",
    )(tables, diag_inv.reshape(supers, parts, cols, share, depth), post)


def apply_lower(tables, base, top, gathered, diag_inv, post, mean, square, keep_y):
    count, height, full = gathered.shape
    _, _, depth = diag_inv.shape
    rhs = post.shape[1]

    def kernel(at, left, lower, post_of, mean_in, square_in, mean_out, square_out, *rest):
        e = pl.program_id(0)
        row = lax.axis_index("row")
        total = rest[-1]

        @pl.when(e == 0)
        def _():
            square_out[...] = square_in[...]

        fill_total(total, left, lower, row)
        found = -total[...]
        if keep_y:
            rest[0][0] = found
        mean_out[0] = mean_in[0] + triple(split(post_of[0]), split(found))
        square_out[pl.ds(at[base + e], 1)] += square_sum(found)

    mean_spec = pl.BlockSpec((1, rhs, depth), lambda e, at: (at[base + e], 0, 0))
    square_spec = pl.BlockSpec(square.shape, lambda e, at: (0, 0))
    out_specs = [mean_spec, square_spec]
    out_shape = [jax.ShapeDtypeStruct(mean.shape, F32), jax.ShapeDtypeStruct(square.shape, F32)]
    if keep_y:
        out_specs.append(pl.BlockSpec((1, height, depth), lambda e, at: (e, 0, 0)))
        out_shape.append(jax.ShapeDtypeStruct((count, height, depth), F32))
    return pl.pallas_call(
        kernel,
        grid_spec=pltpu.PrefetchScalarGridSpec(
            num_scalar_prefetch=1,
            grid=(count,),
            in_specs=[
                pl.BlockSpec((1, height, full), lambda e, at: (e, 0, 0)),
                pl.BlockSpec((1, full, depth), lambda e, at: (at[base + e], 0, 0)),
                pl.BlockSpec((1, rhs, height), lambda e, at: (at[top + e], 0, 0)),
                mean_spec,
                square_spec,
            ],
            out_specs=out_specs,
            scratch_shapes=[VMEM((height, depth), F32)],
        ),
        out_shape=out_shape,
        input_output_aliases={4: 0, 5: 1},
        compiler_params=pltpu.CompilerParams(vmem_limit_bytes=COMPUTE_LIMIT),
        name="apply_lower",
    )(tables, gathered, diag_inv, post, mean, square)


def remote(src, dst, send, recv, row, col):
    return pltpu.make_async_remote_copy(
        src_ref=src, dst_ref=dst, send_sem=send, recv_sem=recv, device_id=(row, col), device_id_type=MESH
    )


def redistribute(partial, start, count, lower_only, cuts, post=None, mine=None):
    _, rows, cols, share, width = partial.shape
    tall = rows // CORES
    full = cols * width
    half = full // 2
    sub = share // cuts
    items = count * cuts
    long = cols // WIDE
    wait_lag = 2 if items > 4 else 1
    if mine is not None:
        blocks, block_rows, block_cols = mine.shape
        lots = blocks * 2
        lot_rows = block_rows // 2
        hops = (long - 1) * lots
        per_step = -(-hops // items)

    def kernel(*refs):
        refs = list(refs)
        src = refs.pop(0)
        piece = refs.pop(0) if post is not None else None
        block_in = refs.pop(0) if mine is not None else None
        result = refs.pop(0)
        posted = refs.pop(0) if post is not None else None
        around = refs.pop(0) if mine is not None else None
        d, out, give, own, one, two = refs[:6]
        load_s, store_s, s1, r1, s2, r2, s3, r3, s4, r4, s5, r5, s6, r6 = refs[6:20]
        refs = refs[20:]
        row = lax.axis_index("row")
        col = lax.axis_index("col")
        core = row % CORES
        y = row // CORES
        mate = y * CORES + (1 - core)
        across = (1 - y) * CORES + core
        z = col // WIDE
        x = col % WIDE

        def part(i):
            return i // cuts, pl.ds(pl.multiple_of(i % cuts * sub, 8), sub)

        def load(e):
            return pltpu.make_async_copy(src.at[start + e], d.at[e], load_s.at[e])

        def store(e):
            return pltpu.make_async_copy(out.at[e], result.at[e], store_s.at[e])

        def core_send(i):
            e, span = part(i)
            return remote(d.at[e, :, 1 - core, :, span], one.at[i], s1.at[i], r1.at[i], mate, col)

        def y_send(i):
            return remote(give.at[i], two.at[i], s2.at[i], r2.at[i], across, col)

        def my_cols():
            return pl.ds(pl.multiple_of(col * width, 128), width)

        def col_send(i, step):
            e, span = part(i)
            to = (col + step) % cols
            return remote(
                own.at[i, to], out.at[e, row, span, my_cols()], s3.at[i, step - 1], r3.at[i, step - 1], row, to
            )

        def share_send(i, which, upper, send, recv, to):
            e, span = part(i)
            ref = out.at[e, which, span, pl.ds(half, half)] if upper else out.at[e, which, span]
            return remote(ref, ref, send.at[i], recv.at[i], to, col)

        def mate_send(i):
            return share_send(i, row, False, s4, r4, mate)

        def across_send(i, upper):
            return share_send(i, row, upper, s5, r5, across)

        def forward(i, upper):
            return share_send(i, across, upper, s6, r6, mate)

        def loop(low, high, body):
            def step(i, _):
                body(i)
                return 0

            lax.fori_loop(low, high, step, 0)

        loop(0, count, lambda e: load(e).start())

        if mine is not None:
            up_s, up_r, down_s, down_r, x_s, x_r = refs[:6]

            def lot(block, q):
                return around.at[block, q // 2, pl.ds(pl.multiple_of(q % 2 * lot_rows, 8), lot_rows)]

            def along(q, hop, sign):
                ref = lot((z - sign * hop) * WIDE + x, q)
                sems = (up_s, up_r) if sign > 0 else (down_s, down_r)
                return remote(ref, ref, sems[0].at[q, hop], sems[1].at[q, hop], row, (z + sign) * WIDE + x)

            def sends(hop, sign):
                return (z - hop >= 0) & (z + 1 < long) if sign > 0 else (z + hop < long) & (z >= 1)

            def gets(hop, sign):
                return z - 1 - hop >= 0 if sign > 0 else z + 1 + hop < long

            def beside(q, offset):
                at = (z + offset + long) % long
                ref = lot(at * WIDE + x, q)
                return remote(ref, ref, x_s.at[q, offset], x_r.at[q, offset], row, z * WIDE + (1 - x))

            for p in range(blocks):
                around[col, p] = block_in[p]

            def begin(q):
                for sign in (1, -1):

                    @pl.when(sends(0, sign))
                    def _():
                        along(q, 0, sign).start()

                beside(q, 0).start()

            loop(0, lots, begin)

            def relay(n):
                hop = n // lots
                q = n % lots
                for sign in (1, -1):

                    @pl.when(gets(hop, sign))
                    def _():
                        along(q, hop, sign).wait_recv()

                        @pl.when(sends(hop + 1, sign))
                        def _():
                            along(q, hop + 1, sign).start()

                        beside(q, (long - sign * (hop + 1)) % long).start()

        def begin_edge(e):
            load(e).wait()
            for c in range(cuts):
                core_send(e * cuts + c).start()

        loop(0, count, begin_edge)

        if post is not None:
            sp, rp = refs[:2]

            def post_send(step):
                to_row = (row + step // cols) % rows
                to_col = (col + step % cols) % cols
                return remote(
                    piece.at[to_col], posted.at[row, col], sp.at[step - 1], rp.at[step - 1], to_row, to_col
                )

            posted[row, col] = piece[col]
            loop(1, rows * cols, lambda step: post_send(step).start())

        def send_cols(i):
            e, span = part(i)
            for step in range(1, cols):
                col_send(i, step).start()
            out[e, row, span, my_cols()] = own[i, col]

        def first(i):
            e, span = part(i)
            core_send(i).wait_recv()
            if lower_only:

                @pl.when(y == 0)
                def _():
                    give[i] = d[e, 1, core, :, span] + one[i, 1]
                    y_send(i).start()
                    own[i] = d[e, 0, core, :, span] + one[i, 0]
                    send_cols(i)
            else:
                give[i] = d[e, 1 - y, core, :, span] + one[i, 1 - y]
                y_send(i).start()

        loop(0, items, first)

        def second(i):
            e, span = part(i)
            if lower_only:

                @pl.when(y == 1)
                def _():
                    y_send(i).wait_recv()
                    own[i] = d[e, 1, core, :, span] + (one[i, 1] + two[i])
                    send_cols(i)
            else:
                y_send(i).wait_recv()
                own[i] = d[e, y, core, :, span] + (one[i, y] + two[i])
                send_cols(i)

        def third(i):
            for step in range(1, cols):
                col_send(i, step).wait_recv()

            @pl.when(y == 0)
            def _():
                across_send(i, True).start()

            @pl.when(y == 1)
            def _():
                across_send(i, False).start()

            mate_send(i).start()

        def fourth(i):
            @pl.when(y == 0)
            def _():
                across_send(i, False).wait_recv()
                forward(i, False).start()

            @pl.when(y == 1)
            def _():
                across_send(i, True).wait_recv()
                forward(i, True).start()

        def stages(t):
            for lag, stage in ((0, second), (wait_lag, third)):

                @pl.when((t >= lag) & (t < items + lag))
                def _():
                    stage(t - lag)

            if mine is not None:
                for k in range(per_step):

                    @pl.when(t * per_step + k < hops)
                    def _():
                        relay(t * per_step + k)

        loop(0, items + wait_lag, stages)
        loop(0, items, fourth)

        def finish(i):
            core_send(i).wait_send()
            if lower_only:

                @pl.when(y == 0)
                def _():
                    y_send(i).wait_send()
            else:
                y_send(i).wait_send()
            for step in range(1, cols):
                col_send(i, step).wait_send()
            mate_send(i).wait()

            @pl.when(y == 0)
            def _():
                across_send(i, True).wait_send()
                forward(i, False).wait()

            @pl.when(y == 1)
            def _():
                across_send(i, False).wait_send()
                forward(i, True).wait()

        def finish_edge(e):
            for c in range(cuts):
                finish(e * cuts + c)
            store(e).start()

        loop(0, count, finish_edge)

        if post is not None:
            loop(1, rows * cols, lambda step: post_send(step).wait())

        if mine is not None:

            def end(q):
                for offset in range(long):
                    beside(q, offset).wait()
                for hop in range(long - 1):
                    for sign in (1, -1):

                        @pl.when(sends(hop, sign))
                        def _():
                            along(q, hop, sign).wait_send()

            loop(0, lots, end)

        loop(0, count, lambda e: store(e).wait())

    spec = pl.BlockSpec(memory_space=VMEM)
    anywhere = pl.BlockSpec(memory_space=pl.ANY)
    dma = pltpu.SemaphoreType.DMA
    in_specs, out_specs = [anywhere], [anywhere]
    out_shape = [jax.ShapeDtypeStruct((count, rows, share, full), F32)]
    args = [partial.reshape(-1, tall, CORES, cols, share, width)]
    scratch = [
        VMEM((count, tall, CORES, cols, share, width), F32),
        VMEM((count, rows, share, full), F32),
        VMEM((items, cols, sub, width), F32),
        VMEM((items, cols, sub, width), F32),
        VMEM((items, tall, cols, sub, width), F32),
        VMEM((items, cols, sub, width), F32),
    ]
    scratch += [dma((count,))] * 2 + [dma((items,))] * 4 + [dma((items, cols - 1))] * 2 + [dma((items,))] * 6
    if post is not None:
        out_shape.append(jax.ShapeDtypeStruct((rows,) + post.shape, F32))
        in_specs.append(spec)
        out_specs.append(spec)
        args.append(post)
        scratch += [dma((rows * cols - 1,))] * 2
    if mine is not None:
        out_shape.append(jax.ShapeDtypeStruct((cols, 2) + mine.shape[1:], F32))
        in_specs.append(spec)
        out_specs.append(spec)
        args.append(mine)
        scratch += [dma((lots, long - 1))] * 4 + [dma((lots, long))] * 2
    return pl.pallas_call(
        kernel,
        out_shape=out_shape,
        in_specs=in_specs,
        out_specs=out_specs,
        scratch_shapes=scratch,
        compiler_params=pltpu.CompilerParams(vmem_limit_bytes=VMEM_LIMIT, has_side_effects=True),
        name="redistribute",
    )(*args)


def scatter_sum(mean, square, cols):
    supers, rhs, depth = mean.shape
    own = rhs // cols

    def kernel(src, sq, out, sq_out, landed, sq_landed, send, recv, sq_send, sq_recv):
        row = lax.axis_index("row")
        col = lax.axis_index("col")

        def piece(c):
            return pl.ds(pl.multiple_of(c * own, own), own)

        def copy(step):
            to = (col + step) % cols
            return remote(
                src.at[:, piece(to)], landed.at[step - 1], send.at[step - 1], recv.at[step - 1], row, to
            )

        def sq_copy(step):
            to = (col + step) % cols
            return remote(sq, sq_landed.at[step - 1], sq_send.at[step - 1], sq_recv.at[step - 1], row, to)

        for step in range(1, cols):
            copy(step).start()
            sq_copy(step).start()
        total = src[:, piece(col)]
        sq_total = sq[...]
        for step in range(1, cols):
            copy(step).wait_recv()
            sq_copy(step).wait_recv()
            total += landed[step - 1]
            sq_total += sq_landed[step - 1]
        out[...] = total
        sq_out[...] = sq_total
        for step in range(1, cols):
            copy(step).wait_send()
            sq_copy(step).wait_send()

    spec = pl.BlockSpec(memory_space=VMEM)
    dma = pltpu.SemaphoreType.DMA
    return pl.pallas_call(
        kernel,
        out_shape=[
            jax.ShapeDtypeStruct((supers, own, depth), F32),
            jax.ShapeDtypeStruct(square.shape, F32),
        ],
        in_specs=[spec, spec],
        out_specs=[spec, spec],
        scratch_shapes=[
            VMEM((cols - 1, supers, own, depth), F32),
            VMEM((cols - 1,) + square.shape, F32),
        ]
        + [dma((cols - 1,))] * 4,
        compiler_params=pltpu.CompilerParams(vmem_limit_bytes=VMEM_LIMIT, has_side_effects=True),
        name="scatter_sum",
    )(mean, square)


def fast_body(rows, cols, factor, diag_inv, structure, parent, post):
    supers, row_width, _, col_width = factor.shape
    full = diag_inv.shape[1]
    last = supers - 1
    share = row_width // cols
    height = rows * share
    rhs_own = post.shape[2]
    rhs = rhs_own * cols

    tables = index_tables(parent)
    flags = structure.reshape(-1)
    blocks = jnp.transpose(factor, (0, 2, 1, 3))

    pieces = jnp.transpose(post.reshape(supers, cols, share, rhs_own), (1, 0, 3, 2))
    pieces = pieces.reshape(cols, supers * rhs_own * share // 128, 128)

    partial = near_partial(tables, flags, diag_inv, blocks)
    partial = partial.reshape(last, rows, cols, share, col_width)

    def near_steps(count, tables, partial, pieces):
        gathered, posted = redistribute(partial, 0, count, True, 4 // count, post=pieces)
        posted = posted.reshape(rows, cols, supers, rhs_own, share)
        posted = jnp.transpose(posted, (2, 1, 3, 0, 4)).reshape(supers, rhs, height)
        mean, square = own_terms(tables, diag_inv, posted)
        gathered = gathered.reshape(count, height, full)
        mean, square, near = apply_lower(
            tables, NEAR, NEAR_TOP, gathered, diag_inv, posted, mean, square, True
        )
        gathered, near_all = redistribute(partial, count, last - count, True, 2, mine=near)
        gathered = gathered.reshape(last - count, height, full)
        mean, square = apply_lower(
            tables, NEAR + count, NEAR_TOP + count, gathered, diag_inv, posted, mean, square, False
        )
        return near_all, posted, mean, square

    branches = [functools.partial(near_steps, count) for count in (1, 2)]
    near_all, posted, mean, square = lax.switch(tables[COUNTS + 1] - 1, branches, tables, partial, pieces)

    def far_steps(count, tables, near_all, posted, mean, square):
        partial = far_partial(tables, flags, near_all, diag_inv, blocks, count)
        partial = partial.reshape(count, rows, cols, share, col_width)
        (gathered,) = redistribute(partial, 0, count, False, 4 if count == 1 else 2)
        gathered = gathered.reshape(count, height, full)
        return apply_lower(tables, FAR, FAR_TOP, gathered, diag_inv, posted, mean, square, False)

    branches = [functools.partial(far_steps, count) for count in range(1, supers - 1)]
    mean, square = lax.switch(tables[COUNTS] - 1, branches, tables, near_all, posted, mean, square)
    mean, square = scatter_sum(mean, square, cols)
    return jnp.swapaxes(mean, 1, 2), square[:supers]


def solution(mesh):
    rows, cols = mesh.shape["row"], mesh.shape["col"]

    def choose(factor, diag_inv, structure, parent, post):
        shapes_fit = (
            rows == 2 * CORES
            and factor.shape[3] % 128 == 0
            and factor.shape[1] % (32 * cols) == 0
            and post.shape[2] % 8 == 0
        )
        if shapes_fit:
            return fast_body(rows, cols, factor, diag_inv, structure, parent, post)
        return body(factor, diag_inv, structure, parent, post)

    return jax.shard_map(
        choose,
        mesh=mesh,
        in_specs=(
            P(None, "row", None, "col"),
            P(None, None, "row"),
            P(None, None, "row"),
            P(),
            P(None, "row", "col"),
        ),
        out_specs=(P(None, "row", "col"), P(None, "row")),
        check_vma=False,
    )
```

```python
import functools

import jax
import jax.numpy as jnp
from jax import lax
from jax.experimental import pallas as pl
from jax.experimental.pallas import tpu as pltpu
from jax.sharding import PartitionSpec as P

HIGH = lax.Precision.HIGH
MESH = pl.DeviceIdType.MESH
F32 = jnp.float32
BF16 = jnp.bfloat16
VMEM = pltpu.VMEM
VMEM_LIMIT = 64 * 1000 * 1024
COMPUTE_LIMIT = 64 * 1000 * 1024
CORES = 2
WIDE = 2


def product(left, right):
    return jnp.dot(left, right, precision=HIGH, preferred_element_type=jnp.float32)


def body(factor, diag_inv, structure, parent, post):
    super_count = factor.shape[0]
    row_width = factor.shape[1]
    col_width = factor.shape[3]
    full_width = diag_inv.shape[1]
    row_at = lax.axis_index("row")
    col_at = lax.axis_index("col")
    last = super_count - 1
    block_rows = row_width // structure.shape[2]

    extended = jnp.concatenate([parent, jnp.full((1,), super_count, jnp.int32)])
    first_at = parent
    second_at = extended[parent]

    def pick(current_sup, target):
        clamped = jnp.minimum(target, last)
        block = lax.dynamic_index_in_dim(factor[:, :, current_sup, :], clamped, 0, keepdims=False)
        flags = lax.dynamic_index_in_dim(structure[current_sup], clamped, 0, keepdims=False)
        flags = jnp.where(target < super_count, flags.astype(jnp.float32), 0.0)
        return block * jnp.repeat(flags, block_rows)[:, None]

    blocks = [None] * super_count
    for current_sup in range(last - 1, -1, -1):
        mine = jnp.concatenate(
            [pick(current_sup, first_at[current_sup]), pick(current_sup, second_at[current_sup])], axis=0
        )
        blocks[current_sup] = lax.all_gather(mine, "col", axis=1, tiled=True)

    own_cols = row_at * row_width + jnp.arange(row_width, dtype=jnp.int32)
    rows_full = jnp.arange(full_width, dtype=jnp.int32)
    keep = rows_full[:, None] >= own_cols[None, :]
    lower = [jnp.where(keep, diag_inv[s], 0.0) for s in range(super_count)]
    unit_rows = col_at * col_width + jnp.arange(col_width, dtype=jnp.int32)
    own = lax.dynamic_slice_in_dim(diag_inv, col_at * col_width, col_width, axis=1)
    own = jnp.where((unit_rows[:, None] >= own_cols[None, :])[None], own, 0.0)
    gathered = jnp.swapaxes(lax.all_gather(post, "row", axis=1, tiled=True), 1, 2)

    def take(stacked, target):
        return lax.dynamic_index_in_dim(stacked, jnp.minimum(target, last), 0, keepdims=False)

    rhs = jnp.stack([product(gathered[s], lower[s]) for s in range(super_count)])

    def solve(current_sup, unit_part, rhs_part):
        summed = lax.psum(jnp.concatenate([unit_part, rhs_part], axis=0), "row")
        right = jnp.concatenate(
            [-summed[:col_width], gathered[current_sup] - summed[col_width:]], axis=0
        )
        fresh = product(right, lower[current_sup])
        return fresh[:col_width], fresh[col_width:]

    near = [jnp.zeros((col_width, row_width), jnp.float32)] * super_count
    means = [rhs[s] for s in range(super_count)]
    for s in range(last - 1, -1, -1):
        one, two = first_at[s], second_at[s]
        unit_part = product(take(own, one), blocks[s][:row_width])
        rhs_part = product(
            jnp.concatenate([take(rhs, one), take(rhs, two)], axis=1), blocks[s]
        )
        near[s], means[s] = solve(s, unit_part, rhs_part)
    near_all = jnp.stack(near)
    rhs = jnp.stack(means)

    far = [None] * super_count
    for s in range(last - 1, -1, -1):
        one, two = first_at[s], second_at[s]
        selected = jnp.concatenate(
            [
                jnp.concatenate([take(near_all, one), take(own, two)], axis=1),
                jnp.concatenate([take(rhs, one), take(rhs, two)], axis=1),
            ],
            axis=0,
        )
        both = product(selected, blocks[s])
        far[s], means[s] = solve(s, both[:col_width], both[col_width:])

    squares = []
    for s in range(super_count):
        total = jnp.sum(own[s] * own[s], axis=0)
        if s < last:
            total = total + jnp.sum(near[s] * near[s], axis=0) + jnp.sum(far[s] * far[s], axis=0)
        squares.append(total)
    variance = lax.psum(jnp.stack(squares), "col")
    mean_x = jnp.swapaxes(jnp.stack(means), 1, 2)
    return (mean_x, variance)


def split(x):
    high = x.astype(BF16)
    return high, (x - high.astype(F32)).astype(BF16)


def triple(a, b):
    left = jnp.concatenate([a[0], a[0], a[1]], axis=1)
    right = jnp.concatenate([b[0], b[1], b[0]], axis=0)
    return jnp.dot(left, right, preferred_element_type=F32)


def triangle(block, row_start, col_start):
    rows = lax.broadcasted_iota(jnp.int32, block.shape, 0) + row_start
    cols = lax.broadcasted_iota(jnp.int32, block.shape, 1) + col_start
    return jnp.where(rows >= cols, block, 0.0)


FIRST, KEPT, FAR, FAR_TOP, FAR_SLOT, FAR_MID, NEAR, NEAR_TOP, COUNTS = 0, 8, 16, 24, 32, 40, 48, 56, 64


def index_tables(parent):
    supers = parent.shape[0]
    last = supers - 1

    def kernel(up, out):
        for i in range(72):
            out[i] = 0
        firsts = [jnp.minimum(up[s], last) for s in range(supers)]
        count = jnp.int32(0)
        low = jnp.int32(last)
        high = jnp.int32(0)
        for s in range(supers):
            out[FIRST + s] = firsts[s]
            out[KEPT + s] = jnp.where(up[s] < supers, 1, 0)
        for s in range(supers):
            far = (up[s] < supers) & (up[firsts[s]] < supers)
            low = jnp.where(far, jnp.minimum(low, firsts[s]), low)
            high = jnp.where(far, jnp.maximum(high, firsts[s]), high)
        for s in range(supers):
            top = up[firsts[s]]
            far = (up[s] < supers) & (top < supers)

            @pl.when(far)
            def _():
                out[FAR + count] = s
                out[FAR_TOP + count] = top
                out[FAR_SLOT + count] = jnp.where(firsts[s] == low, 0, 1)
                out[FAR_MID + count] = firsts[s]

            count = count + jnp.where(far, 1, 0)
        out[COUNTS] = count
        out[COUNTS + 1] = jnp.where(low < high, 2, 1)
        out[COUNTS + 2] = lax.axis_index("col")
        place = jnp.int32(0)
        for middle in (True, False):
            for s in range(last):
                between = (low == s) | (high == s)
                now = between if middle else jnp.logical_not(between)

                @pl.when(now)
                def _():
                    out[NEAR + place] = s
                    out[NEAR_TOP + place] = firsts[s]

                place = place + jnp.where(now, 1, 0)

    smem = pl.BlockSpec(memory_space=pltpu.SMEM)
    return pl.pallas_call(
        kernel,
        out_shape=jax.ShapeDtypeStruct((72,), jnp.int32),
        in_specs=[smem],
        out_specs=smem,
        name="index_tables",
    )(parent)


def masked(block, flags, s, t, supers, scale):
    depth = block.shape[0]
    pieces = flags.shape[0] // (supers * supers)
    size = depth // pieces
    kept = []
    for b in range(pieces):
        flag = (flags[(s * supers + t) * pieces + b] * scale).astype(F32)
        kept.append(block[b * size : (b + 1) * size] * flag)
    return jnp.concatenate(kept, axis=0)


def near_partial(tables, flags, diag_inv, factor):
    supers, _, depth, width = factor.shape
    full = diag_inv.shape[1]
    parts = full // depth
    count = supers - 1

    def kernel(at, keep, lower, block, out):
        e = pl.program_id(0)
        row = lax.axis_index("row")
        s = at[NEAR + e]
        right = split(masked(block[0, 0], keep, s, at[NEAR_TOP + e], supers, at[KEPT + s]))

        def below(i, _):
            span = pl.ds(pl.multiple_of(i * depth, 8), depth)
            left = triangle(lower[0, span], i * depth, row * depth)
            out[0, span] = triple(split(left), right)
            return 0

        def above(i, _):
            span = pl.ds(pl.multiple_of(i * depth, 8), depth)
            out[0, span] = jnp.zeros((depth, width), F32)
            return 0

        lax.fori_loop(row, parts, below, 0)
        lax.fori_loop(0, row, above, 0)

    return pl.pallas_call(
        kernel,
        grid_spec=pltpu.PrefetchScalarGridSpec(
            num_scalar_prefetch=2,
            grid=(count,),
            in_specs=[
                pl.BlockSpec((1, full, depth), lambda e, at, keep: (at[NEAR_TOP + e], 0, 0)),
                pl.BlockSpec((1, 1, depth, width), lambda e, at, keep: (at[NEAR_TOP + e], at[NEAR + e], 0, 0)),
            ],
            out_specs=pl.BlockSpec((1, full, width), lambda e, at, keep: (e, 0, 0)),
        ),
        out_shape=jax.ShapeDtypeStruct((count, full, width), F32),
        compiler_params=pltpu.CompilerParams(vmem_limit_bytes=COMPUTE_LIMIT),
        name="near_partial",
    )(tables, flags, diag_inv, factor)


def far_partial(tables, flags, near_all, diag_inv, factor, count):
    supers, _, depth, width = factor.shape
    full = diag_inv.shape[1]
    parts = full // depth
    cols = near_all.shape[0]
    share = depth // cols

    def kernel(at, keep, near, lower, one, two, out):
        e = pl.program_id(0)
        row = lax.axis_index("row")
        s = at[FAR + e]
        left_one = split(masked(one[0, 0], keep, s, at[FAR_MID + e], supers, 1))
        left_two = split(masked(two[0, 0], keep, s, at[FAR_TOP + e], supers, 1))

        def dense(i, _):
            span = pl.ds(pl.multiple_of(i * depth, 8), depth)
            rows = near[:, 0, pl.ds(pl.multiple_of(i * share, 8), share)].reshape(depth, depth)
            out[0, span] = triple(split(rows), left_one)
            return 0

        def below(i, _):
            span = pl.ds(pl.multiple_of(i * depth, 8), depth)
            left = triangle(lower[0, span], i * depth, row * depth)
            out[0, span] += triple(split(left), left_two)
            return 0

        lax.fori_loop(0, parts, dense, 0)
        lax.fori_loop(row, parts, below, 0)

    return pl.pallas_call(
        kernel,
        grid_spec=pltpu.PrefetchScalarGridSpec(
            num_scalar_prefetch=2,
            grid=(count,),
            in_specs=[
                pl.BlockSpec((cols, 1, parts * share, depth), lambda e, at, keep: (0, at[FAR_SLOT + e], 0, 0)),
                pl.BlockSpec((1, full, depth), lambda e, at, keep: (at[FAR_TOP + e], 0, 0)),
                pl.BlockSpec((1, 1, depth, width), lambda e, at, keep: (at[FAR_MID + e], at[FAR + e], 0, 0)),
                pl.BlockSpec((1, 1, depth, width), lambda e, at, keep: (at[FAR_TOP + e], at[FAR + e], 0, 0)),
            ],
            out_specs=pl.BlockSpec((1, full, width), lambda e, at, keep: (e, 0, 0)),
        ),
        out_shape=jax.ShapeDtypeStruct((count, full, width), F32),
        compiler_params=pltpu.CompilerParams(vmem_limit_bytes=COMPUTE_LIMIT),
        name="far_partial",
    )(tables, flags, near_all, diag_inv, factor, factor)


def unfold(post):
    rows, cols, _, rhs_own, share = post.shape
    return jnp.concatenate([post[i].reshape(cols * rhs_own, share) for i in range(rows)], axis=1)


def square_sum(found):
    return jnp.sum(found * found, axis=0, keepdims=True)


def fill_total(total, left, lower, row):
    depth = lower.shape[2]
    parts = left.shape[2] // depth
    total[...] = jnp.zeros_like(total)

    def add(j, _):
        span = pl.ds(pl.multiple_of(j * depth, 128), depth)
        right = triangle(lower[0, span], j * depth, row * depth)
        total[...] += triple(split(left[0, :, span]), split(right))
        return 0

    lax.fori_loop(row, parts, add, 0)


def own_terms(tables, diag_inv, post):
    supers, full, depth = diag_inv.shape
    parts, cols, _, rhs_own, share = post.shape
    rhs = cols * rhs_own
    lines = supers + -supers % 8

    def kernel(at, lower, post_own, mean, square):
        e = pl.program_id(0)
        row = lax.axis_index("row")
        col = lax.axis_index("col")
        rows = [
            triangle(lower[0, i, 0], i * depth + col * share, row * depth) for i in range(parts)
        ]
        own = jnp.concatenate(rows, axis=0)
        mean[0] = triple(split(unfold(post_own[...])), split(own))
        square[pl.ds(e, 1)] = square_sum(own)

    return pl.pallas_call(
        kernel,
        grid_spec=pltpu.PrefetchScalarGridSpec(
            num_scalar_prefetch=1,
            grid=(supers,),
            in_specs=[
                pl.BlockSpec((1, parts, 1, share, depth), lambda e, at: (e, 0, at[COUNTS + 2], 0, 0)),
                pl.BlockSpec((parts, cols, 1, rhs_own, share), lambda e, at: (0, 0, e, 0, 0)),
            ],
            out_specs=[
                pl.BlockSpec((1, rhs, depth), lambda e, at: (e, 0, 0)),
                pl.BlockSpec((lines, depth), lambda e, at: (0, 0)),
            ],
        ),
        out_shape=[
            jax.ShapeDtypeStruct((supers, rhs, depth), F32),
            jax.ShapeDtypeStruct((lines, depth), F32),
        ],
        compiler_params=pltpu.CompilerParams(vmem_limit_bytes=COMPUTE_LIMIT),
        name="own_terms",
    )(tables, diag_inv.reshape(supers, parts, cols, share, depth), post)


def apply_lower(tables, base, top, gathered, diag_inv, post, mean, square, keep_y):
    count, height, full = gathered.shape
    _, _, depth = diag_inv.shape
    rows, cols, _, rhs_own, share = post.shape
    rhs = cols * rhs_own
    fresh = mean is None

    def kernel(at, left, lower, post_of, square_in, *rest):
        rest = list(rest)
        mean_in = None if fresh else rest.pop(0)
        mean_out, square_out = rest[:2]
        e = pl.program_id(0)
        row = lax.axis_index("row")
        total = rest[-1]

        @pl.when(e == 0)
        def _():
            square_out[...] = square_in[...]

        fill_total(total, left, lower, row)
        found = -total[...]
        if keep_y:
            rest[2][0] = found
        term = triple(split(unfold(post_of[...])), split(found))
        mean_out[0] = term if fresh else mean_in[0] + term
        square_out[pl.ds(at[base + e], 1)] += square_sum(found)

    if fresh:
        mean_spec = pl.BlockSpec((1, rhs, depth), lambda e, at: (e, 0, 0))
        mean_shape = jax.ShapeDtypeStruct((count, rhs, depth), F32)
    else:
        mean_spec = pl.BlockSpec((1, rhs, depth), lambda e, at: (at[base + e], 0, 0))
        mean_shape = jax.ShapeDtypeStruct(mean.shape, F32)
    square_spec = pl.BlockSpec(square.shape, lambda e, at: (0, 0))
    in_specs = [
        pl.BlockSpec((1, height, full), lambda e, at: (e, 0, 0)),
        pl.BlockSpec((1, full, depth), lambda e, at: (at[base + e], 0, 0)),
        pl.BlockSpec((rows, cols, 1, rhs_own, share), lambda e, at: (0, 0, at[top + e], 0, 0)),
        square_spec,
    ]
    out_specs = [mean_spec, square_spec]
    out_shape = [mean_shape, jax.ShapeDtypeStruct(square.shape, F32)]
    aliases = {4: 1}
    args = [tables, gathered, diag_inv, post, square]
    if not fresh:
        in_specs.append(mean_spec)
        args.append(mean)
        aliases[5] = 0
    if keep_y:
        out_specs.append(pl.BlockSpec((1, height, depth), lambda e, at: (e, 0, 0)))
        out_shape.append(jax.ShapeDtypeStruct((count, height, depth), F32))
    return pl.pallas_call(
        kernel,
        grid_spec=pltpu.PrefetchScalarGridSpec(
            num_scalar_prefetch=1,
            grid=(count,),
            in_specs=in_specs,
            out_specs=out_specs,
            scratch_shapes=[VMEM((height, depth), F32)],
        ),
        out_shape=out_shape,
        input_output_aliases=aliases,
        compiler_params=pltpu.CompilerParams(vmem_limit_bytes=COMPUTE_LIMIT),
        name="apply_lower",
    )(*args)


def remote(src, dst, send, recv, row, col):
    return pltpu.make_async_remote_copy(
        src_ref=src, dst_ref=dst, send_sem=send, recv_sem=recv, device_id=(row, col), device_id_type=MESH
    )


def redistribute(partial, start, count, lower_only, cuts, post=None, mine=None, sums=None):
    _, rows, cols, share, width = partial.shape
    tall = rows // CORES
    full = cols * width
    half = full // 2
    sub = share // cuts
    items = count * cuts
    long = cols // WIDE
    wait_lag = 2 if items > 4 else 1
    if mine is not None:
        blocks, block_rows, block_cols = mine.shape
        lots = blocks * 2
        lot_rows = block_rows // 2
        hops = (long - 1) * lots
        per_step = -(-hops // items)

    def kernel(*refs):
        refs = list(refs)
        src = refs.pop(0)
        piece = refs.pop(0) if post is not None else None
        block_in = refs.pop(0) if mine is not None else None
        sums_in = refs.pop(0) if sums is not None else None
        result = refs.pop(0)
        posted = refs.pop(0) if post is not None else None
        around = refs.pop(0) if mine is not None else None
        sums_out = refs.pop(0) if sums is not None else None
        d, out, give, own, one, two = refs[:6]
        load_s, store_s, s1, r1, s2, r2, s3, r3, s4, r4, s5, r5, s6, r6 = refs[6:20]
        refs = refs[20:]
        row = lax.axis_index("row")
        col = lax.axis_index("col")
        core = row % CORES
        y = row // CORES
        mate = y * CORES + (1 - core)
        across = (1 - y) * CORES + core
        z = col // WIDE
        x = col % WIDE

        def part(i):
            return i // cuts, pl.ds(pl.multiple_of(i % cuts * sub, 8), sub)

        def load(e):
            return pltpu.make_async_copy(src.at[start + e], d.at[e], load_s.at[e])

        def store(e):
            return pltpu.make_async_copy(out.at[e], result.at[e], store_s.at[e])

        def core_send(i):
            e, span = part(i)
            return remote(d.at[e, :, 1 - core, :, span], one.at[i], s1.at[i], r1.at[i], mate, col)

        def y_send(i):
            return remote(give.at[i], two.at[i], s2.at[i], r2.at[i], across, col)

        def my_cols():
            return pl.ds(pl.multiple_of(col * width, 128), width)

        def col_send(i, step):
            e, span = part(i)
            to = (col + step) % cols
            return remote(
                own.at[i, to], out.at[e, row, span, my_cols()], s3.at[i, step - 1], r3.at[i, step - 1], row, to
            )

        def share_send(i, which, upper, send, recv, to):
            e, span = part(i)
            ref = out.at[e, which, span, pl.ds(half, half)] if upper else out.at[e, which, span]
            return remote(ref, ref, send.at[i], recv.at[i], to, col)

        def mate_send(i):
            return share_send(i, row, False, s4, r4, mate)

        def across_send(i, upper):
            return share_send(i, row, upper, s5, r5, across)

        def forward(i, upper):
            return share_send(i, across, upper, s6, r6, mate)

        def loop(low, high, body):
            def step(i, _):
                body(i)
                return 0

            lax.fori_loop(low, high, step, 0)

        loop(0, count, lambda e: load(e).start())

        if mine is not None:
            up_s, up_r, down_s, down_r, x_s, x_r = refs[:6]

            def lot(block, q):
                return around.at[block, q // 2, pl.ds(pl.multiple_of(q % 2 * lot_rows, 8), lot_rows)]

            def along(q, hop, sign):
                ref = lot((z - sign * hop) * WIDE + x, q)
                sems = (up_s, up_r) if sign > 0 else (down_s, down_r)
                return remote(ref, ref, sems[0].at[q, hop], sems[1].at[q, hop], row, (z + sign) * WIDE + x)

            def sends(hop, sign):
                return (z - hop >= 0) & (z + 1 < long) if sign > 0 else (z + hop < long) & (z >= 1)

            def gets(hop, sign):
                return z - 1 - hop >= 0 if sign > 0 else z + 1 + hop < long

            def beside(q, offset):
                at = (z + offset + long) % long
                ref = lot(at * WIDE + x, q)
                return remote(ref, ref, x_s.at[q, offset], x_r.at[q, offset], row, z * WIDE + (1 - x))

            for p in range(blocks):
                around[col, p] = block_in[p]

            def begin(q):
                for sign in (1, -1):

                    @pl.when(sends(0, sign))
                    def _():
                        along(q, 0, sign).start()

                beside(q, 0).start()

            loop(0, lots, begin)

            def relay(n):
                hop = n // lots
                q = n % lots
                for sign in (1, -1):

                    @pl.when(gets(hop, sign))
                    def _():
                        along(q, hop, sign).wait_recv()

                        @pl.when(sends(hop + 1, sign))
                        def _():
                            along(q, hop + 1, sign).start()

                        beside(q, (long - sign * (hop + 1)) % long).start()

        def begin_edge(e):
            load(e).wait()
            for c in range(cuts):
                core_send(e * cuts + c).start()

        loop(0, count, begin_edge)

        if post is not None:
            pc_s, pc_r, pr_s, pr_r = refs[:4]

            def post_col(step):
                to = (col + step) % cols
                return remote(
                    piece.at[to], posted.at[row, col], pc_s.at[step - 1], pc_r.at[step - 1], row, to
                )

            def post_row(step):
                to = (row + step) % rows
                return remote(
                    posted.at[row], posted.at[row], pr_s.at[step - 1], pr_r.at[step - 1], to, col
                )

        if sums is not None:
            landed, su_s, su_r = refs[:3]
            own_sum = sums_in.shape[1] // cols

            def sum_piece(c):
                return pl.ds(pl.multiple_of(c * own_sum, 8), own_sum)

            def sum_send(step):
                to = (col + step) % cols
                return remote(
                    sums_in.at[:, sum_piece(to)], landed.at[step - 1], su_s.at[step - 1], su_r.at[step - 1], row, to
                )

        def send_cols(i):
            e, span = part(i)
            for step in range(1, cols):
                col_send(i, step).start()
            out[e, row, span, my_cols()] = own[i, col]

        def first(i):
            e, span = part(i)
            core_send(i).wait_recv()
            if lower_only:

                @pl.when(y == 0)
                def _():
                    give[i] = d[e, 1, core, :, span] + one[i, 1]
                    y_send(i).start()
                    own[i] = d[e, 0, core, :, span] + one[i, 0]
                    send_cols(i)
            else:
                give[i] = d[e, 1 - y, core, :, span] + one[i, 1 - y]
                y_send(i).start()

        loop(0, items, first)

        if post is not None:
            posted[row, col] = piece[col]
            loop(1, cols, lambda step: post_col(step).start())

        def second(i):
            e, span = part(i)
            if lower_only:

                @pl.when(y == 1)
                def _():
                    y_send(i).wait_recv()
                    own[i] = d[e, 1, core, :, span] + (one[i, 1] + two[i])
                    send_cols(i)
            else:
                y_send(i).wait_recv()
                own[i] = d[e, y, core, :, span] + (one[i, y] + two[i])
                send_cols(i)

        def third(i):
            for step in range(1, cols):
                col_send(i, step).wait_recv()

            @pl.when(y == 0)
            def _():
                across_send(i, True).start()

            @pl.when(y == 1)
            def _():
                across_send(i, False).start()

            mate_send(i).start()

        def fourth(i):
            @pl.when(y == 0)
            def _():
                across_send(i, False).wait_recv()
                forward(i, False).start()

            @pl.when(y == 1)
            def _():
                across_send(i, True).wait_recv()
                forward(i, True).start()

        def stages(t):
            for lag, stage in ((0, second), (wait_lag, third)):

                @pl.when((t >= lag) & (t < items + lag))
                def _():
                    stage(t - lag)

            if mine is not None:
                for k in range(per_step):

                    @pl.when(t * per_step + k < hops)
                    def _():
                        relay(t * per_step + k)

        loop(0, items + wait_lag, stages)

        if post is not None:
            loop(1, cols, lambda step: post_col(step).wait_recv())
            loop(1, rows, lambda step: post_row(step).start())

        if sums is not None:
            loop(1, cols, lambda step: sum_send(step).start())

        loop(0, items, fourth)

        def finish(i):
            core_send(i).wait_send()
            if lower_only:

                @pl.when(y == 0)
                def _():
                    y_send(i).wait_send()
            else:
                y_send(i).wait_send()
            for step in range(1, cols):
                col_send(i, step).wait_send()
            mate_send(i).wait()

            @pl.when(y == 0)
            def _():
                across_send(i, True).wait_send()
                forward(i, False).wait()

            @pl.when(y == 1)
            def _():
                across_send(i, False).wait_send()
                forward(i, True).wait()

        def finish_edge(e):
            for c in range(cuts):
                finish(e * cuts + c)
            store(e).start()

        loop(0, count, finish_edge)

        if post is not None:
            loop(1, cols, lambda step: post_col(step).wait_send())
            loop(1, rows, lambda step: post_row(step).wait())

        if sums is not None:
            sums_out[...] = sums_in[:, sum_piece(col)]

            def add_sum(step):
                sum_send(step).wait_recv()
                sums_out[...] += landed[step - 1]

            loop(1, cols, add_sum)
            loop(1, cols, lambda step: sum_send(step).wait_send())

        if mine is not None:

            def end(q):
                for offset in range(long):
                    beside(q, offset).wait()
                for hop in range(long - 1):
                    for sign in (1, -1):

                        @pl.when(sends(hop, sign))
                        def _():
                            along(q, hop, sign).wait_send()

            loop(0, lots, end)

        loop(0, count, lambda e: store(e).wait())

    spec = pl.BlockSpec(memory_space=VMEM)
    anywhere = pl.BlockSpec(memory_space=pl.ANY)
    dma = pltpu.SemaphoreType.DMA
    in_specs, out_specs = [anywhere], [anywhere]
    out_shape = [jax.ShapeDtypeStruct((count, rows, share, full), F32)]
    args = [partial.reshape(-1, tall, CORES, cols, share, width)]
    scratch = [
        VMEM((count, tall, CORES, cols, share, width), F32),
        VMEM((count, rows, share, full), F32),
        VMEM((items, cols, sub, width), F32),
        VMEM((items, cols, sub, width), F32),
        VMEM((items, tall, cols, sub, width), F32),
        VMEM((items, cols, sub, width), F32),
    ]
    scratch += [dma((count,))] * 2 + [dma((items,))] * 4 + [dma((items, cols - 1))] * 2 + [dma((items,))] * 6
    if post is not None:
        out_shape.append(jax.ShapeDtypeStruct((rows,) + post.shape, F32))
        in_specs.append(spec)
        out_specs.append(spec)
        args.append(post)
        scratch += [dma((cols - 1,))] * 2 + [dma((rows - 1,))] * 2
    if mine is not None:
        out_shape.append(jax.ShapeDtypeStruct((cols, 2) + mine.shape[1:], F32))
        in_specs.append(spec)
        out_specs.append(spec)
        args.append(mine)
        scratch += [dma((lots, long - 1))] * 4 + [dma((lots, long))] * 2
    if sums is not None:
        share_shape = (sums.shape[0], sums.shape[1] // cols, sums.shape[2])
        out_shape.append(jax.ShapeDtypeStruct(share_shape, F32))
        in_specs.append(spec)
        out_specs.append(spec)
        args.append(sums)
        scratch += [VMEM((cols - 1,) + share_shape, F32)] + [dma((cols - 1,))] * 2
    return pl.pallas_call(
        kernel,
        out_shape=out_shape,
        in_specs=in_specs,
        out_specs=out_specs,
        scratch_shapes=scratch,
        compiler_params=pltpu.CompilerParams(vmem_limit_bytes=VMEM_LIMIT, has_side_effects=True),
        name="redistribute",
    )(*args)


def scatter_sum(mean, square, cols):
    supers, rhs, depth = mean.shape
    own = rhs // cols

    def kernel(src, sq, out, sq_out, landed, sq_landed, send, recv, sq_send, sq_recv):
        row = lax.axis_index("row")
        col = lax.axis_index("col")

        def piece(c):
            return pl.ds(pl.multiple_of(c * own, own), own)

        def copy(step):
            to = (col + step) % cols
            return remote(
                src.at[:, piece(to)], landed.at[step - 1], send.at[step - 1], recv.at[step - 1], row, to
            )

        def sq_copy(step):
            to = (col + step) % cols
            return remote(sq, sq_landed.at[step - 1], sq_send.at[step - 1], sq_recv.at[step - 1], row, to)

        for step in range(1, cols):
            copy(step).start()
            sq_copy(step).start()
        total = src[:, piece(col)]
        sq_total = sq[...]
        for step in range(1, cols):
            copy(step).wait_recv()
            sq_copy(step).wait_recv()
            total += landed[step - 1]
            sq_total += sq_landed[step - 1]
        out[...] = total
        sq_out[...] = sq_total
        for step in range(1, cols):
            copy(step).wait_send()
            sq_copy(step).wait_send()

    spec = pl.BlockSpec(memory_space=VMEM)
    dma = pltpu.SemaphoreType.DMA
    return pl.pallas_call(
        kernel,
        out_shape=[
            jax.ShapeDtypeStruct((supers, own, depth), F32),
            jax.ShapeDtypeStruct(square.shape, F32),
        ],
        in_specs=[spec, spec],
        out_specs=[spec, spec],
        scratch_shapes=[
            VMEM((cols - 1, supers, own, depth), F32),
            VMEM((cols - 1,) + square.shape, F32),
        ]
        + [dma((cols - 1,))] * 4,
        compiler_params=pltpu.CompilerParams(vmem_limit_bytes=VMEM_LIMIT, has_side_effects=True),
        name="scatter_sum",
    )(mean, square)


def add_far(tables, far, mean):
    count = far.shape[0]

    def kernel(at, far_ref, mean_ref, out):
        out[...] = mean_ref[...]
        for e in range(count):
            out[at[FAR + e]] += far_ref[e]

    spec = pl.BlockSpec(memory_space=VMEM)
    return pl.pallas_call(
        kernel,
        out_shape=jax.ShapeDtypeStruct(mean.shape, F32),
        in_specs=[pl.BlockSpec(memory_space=pltpu.SMEM), spec, spec],
        out_specs=spec,
        name="add_far",
    )(tables, far, mean)


def fast_body(rows, cols, factor, diag_inv, structure, parent, post):
    supers, row_width, _, col_width = factor.shape
    full = diag_inv.shape[1]
    last = supers - 1
    share = row_width // cols
    height = rows * share
    rhs_own = post.shape[2]

    tables = index_tables(parent)
    flags = structure.reshape(-1)
    blocks = jnp.transpose(factor, (0, 2, 1, 3))

    pieces = jnp.transpose(post.reshape(supers, cols, share, rhs_own), (1, 0, 3, 2))

    partial = near_partial(tables, flags, diag_inv, blocks)
    partial = partial.reshape(last, rows, cols, share, col_width)

    def near_steps(count, tables, partial, pieces):
        gathered, posted = redistribute(partial, 0, count, True, 4 // count, post=pieces)
        mean, square = own_terms(tables, diag_inv, posted)
        gathered = gathered.reshape(count, height, full)
        mean, square, near = apply_lower(
            tables, NEAR, NEAR_TOP, gathered, diag_inv, posted, mean, square, True
        )
        gathered, near_all = redistribute(partial, count, last - count, True, 2, mine=near)
        gathered = gathered.reshape(last - count, height, full)
        mean, square = apply_lower(
            tables, NEAR + count, NEAR_TOP + count, gathered, diag_inv, posted, mean, square, False
        )
        return near_all, posted, mean, square

    branches = [functools.partial(near_steps, count) for count in (1, 2)]
    near_all, posted, mean, square = lax.switch(tables[COUNTS + 1] - 1, branches, tables, partial, pieces)

    def far_steps(count, tables, near_all, posted, mean, square):
        partial = far_partial(tables, flags, near_all, diag_inv, blocks, count)
        partial = partial.reshape(count, rows, cols, share, col_width)
        gathered, mean = redistribute(partial, 0, count, False, 4 if count == 1 else 2, sums=mean)
        gathered = gathered.reshape(count, height, full)
        far, square = apply_lower(tables, FAR, FAR_TOP, gathered, diag_inv, posted, None, square, False)
        far, square = scatter_sum(far, square, cols)
        return add_far(tables, far, mean), square[:supers]

    branches = [functools.partial(far_steps, count) for count in range(1, supers - 1)]
    mean, variance = lax.switch(tables[COUNTS] - 1, branches, tables, near_all, posted, mean, square)
    return jnp.swapaxes(mean, 1, 2), variance


def solution(mesh):
    rows, cols = mesh.shape["row"], mesh.shape["col"]

    def choose(factor, diag_inv, structure, parent, post):
        shapes_fit = (
            rows == 2 * CORES
            and factor.shape[3] % 128 == 0
            and factor.shape[1] % (32 * cols) == 0
            and post.shape[2] % 8 == 0
        )
        if shapes_fit:
            return fast_body(rows, cols, factor, diag_inv, structure, parent, post)
        return body(factor, diag_inv, structure, parent, post)

    return jax.shard_map(
        choose,
        mesh=mesh,
        in_specs=(
            P(None, "row", None, "col"),
            P(None, None, "row"),
            P(None, None, "row"),
            P(),
            P(None, "row", "col"),
        ),
        out_specs=(P(None, "row", "col"), P(None, "row")),
        check_vma=False,
    )
```
